32 devices in a mesh: dom: 8 (over z, y), sub: 4 (over x, core).
Axes of the slice: x: 2, y: 2, z: 4, core: 2. Of those that a mesh axis runs over, the one named last changes fastest.
Arguments:
- positions: float32 [3, 131072], P(None, ('dom', 'sub')), may hold values from -20 to 20
- mass: float32 [131072], P(('dom', 'sub')), may hold values from 3 to 6
- local_tiles: float32 [2048, 128, 128], P(('dom', 'sub')), as said below
- local_rows: int32 [2048], P(('dom', 'sub')), may hold values from 0 to 31, as said below
- local_cols: int32 [2048], P(('dom', 'sub')), may hold values from 0 to 31, as said below
- live_tiles: int32 [32], P(('dom', 'sub')), may hold values from 32 to 64, as said below
- dom_tiles: float32 [1024, 128, 128], P(('dom', 'sub')), as said below
- dom_cols: int32 [1024], P(('dom', 'sub')), may hold values from 0 to 31
- dom_slots: int32 [1024], P(('dom', 'sub')), may hold values from 0 to 255, as said below
- dom_rows: int32 [8192], P(('dom', 'sub')), may hold values from 0 to 31, as said below
- sub_tiles: float32 [1536, 128, 128], P(('dom', 'sub')), as said below
- sub_cols: int32 [1536], P(('dom', 'sub')), may hold values from 0 to 31
- sub_slots: int32 [1536], P(('dom', 'sub')), may hold values from 0 to 63, as said below
- sub_rows: int32 [2048], P(('dom', 'sub')), may hold values from 0 to 31, as said below
- precond: float32 [1024, 128, 128], P(('dom', 'sub')), may hold values from -0.05 to 0.3, as said below
Outputs:
- solution: float32 [3, 131072], P(None, ('dom', 'sub'))
- residual: float32 [3, 131072], P(None, ('dom', 'sub'))
The draws below stay inside these ranges and needn't reach their ends.
Inputs may be any that keep to these rules, and one draw needn't show every extreme that they name: Device d uses the first live_tiles[d] of its 64 interior tiles, an even number; some device uses all of them. `local_tiles`: interior tiles come in pairs 2i, 2i + 1 of a device: the second is the transpose of the first. `local_rows`: tile 2i + 1 of a device has the block row and column of tile 2i swapped. `local_cols`: tile 2i + 1 of a device has the block row and column of tile 2i swapped. `dom_slots`: the destination group of a tile differs from its device's dom index in exactly one of its 3 bits; no two tiles of a device share a slot. `dom_rows`: entries for slots that no tile fills are arbitrary blocks of the receiver. `dom_tiles`: every coupling tile that reaches block row r of a device from block column c of another has a transposed tile on the receiver, from its block column r, that reaches block row c of the sender; so A is symmetric. `sub_slots`: the destination partition of a tile lies in its device's group and is not its device's own; no two tiles of a device share a slot. `sub_rows`: entries for slots that no tile fills are arbitrary blocks of the receiver. `sub_tiles`: every such tile has a transposed partner on the receiving partition that is routed back to the sender's block column. `precond`: every block is symmetric and positive definite.
All inputs are finite; a program needn't handle non-finite values.
Results may differ from the reference program's by a relative error of at most 0.0003.
Values sent between devices are 32-bit elements; how exact they have to be, the bound alone decides.
A program may use at most 64 MiB of HBM per device.

```python
import math
import jax
import jax.numpy as jnp
from jax import lax

TILE = 128
DIMS = 3
NB = 32
ITERS = 3
DBITS = 3
LT = 64
IFD = 32
IFS = 48
SD = 32
SS = 16
V_DEV = 4096
VERTS = 131072
N_DOM = 8
N_SUB = 4


def tile_noise(key, shape):
    values = jax.random.normal(key, shape, jnp.float32)
    return jnp.clip(values, -6.0, 6.0) / math.sqrt(8 * TILE)


def draw_positions(key, part):
    devices_all = VERTS // V_DEV
    owners = jnp.arange(VERTS, dtype=jnp.int32) // V_DEV
    scaling = 1.0 + 2.0 * owners.astype(jnp.float32) / max(devices_all - 1, 1)
    base = jnp.clip(jax.random.normal(key, (DIMS, VERTS), jnp.float32), -6.0, 6.0)
    return jnp.clip(base * scaling[None, :], -20.0, 20.0)


def local_plan(key):
    devices_all = VERTS // V_DEV
    subkeys = jax.random.split(jax.random.fold_in(key, 5), 3)
    first_rows = jax.random.randint(subkeys[0], (devices_all * NB,), 0, NB, dtype=jnp.int32)
    first_cols = jax.random.randint(subkeys[1], (devices_all * NB,), 0, NB, dtype=jnp.int32)
    return (first_rows, first_cols, subkeys[2])


def draw_local_tiles(key, part):
    devices_all = VERTS // V_DEV
    first_rows, first_cols, tile_key = local_plan(key)
    halves = tile_noise(tile_key, (devices_all * NB, TILE, TILE))
    paired = jnp.stack([halves, jnp.swapaxes(halves, 1, 2)], axis=1)
    return paired.reshape(devices_all * LT, TILE, TILE)


def draw_local_rows(key, part):
    first_rows, first_cols, tile_key = local_plan(key)
    return jnp.stack([first_rows, first_cols], axis=1).reshape(-1).astype(jnp.int32)


def draw_local_cols(key, part):
    first_rows, first_cols, tile_key = local_plan(key)
    return jnp.stack([first_cols, first_rows], axis=1).reshape(-1).astype(jnp.int32)


def draw_live_tiles(key, part):
    devices_all = VERTS // V_DEV
    first, second = jax.random.split(key)
    values = 2 * jax.random.randint(first, (devices_all,), NB // 2, NB + 1, dtype=jnp.int32)
    chosen = jax.random.randint(second, (), 0, devices_all, dtype=jnp.int32)
    return jnp.where(jnp.arange(devices_all, dtype=jnp.int32) == chosen, LT, values).astype(jnp.int32)


def dom_plan(key):
    devices_all = VERTS // V_DEV
    half = IFD // 2
    subkeys = jax.random.split(jax.random.fold_in(key, 11), 5)
    bit_choice = jax.random.randint(subkeys[0], (N_SUB, half), 0, DBITS, dtype=jnp.int32)
    bit_choice = bit_choice.at[0, 0].set(DBITS - 1)
    cols_up = jax.random.randint(subkeys[1], (devices_all, half), 0, NB, dtype=jnp.int32)
    rows_up = jax.random.randint(subkeys[2], (devices_all, half), 0, NB, dtype=jnp.int32)
    device_ids = jnp.arange(devices_all, dtype=jnp.int32)
    group_of = device_ids // N_SUB
    member_of = device_ids % N_SUB
    flip_dev = jnp.left_shift(jnp.ones((devices_all, half), jnp.int32), bit_choice[member_of])
    source_down = jnp.bitwise_xor(group_of[:, None], flip_dev) * N_SUB + member_of[:, None]
    return (flip_dev, cols_up, rows_up, source_down, group_of, member_of, subkeys[3], subkeys[4])


def draw_dom_tiles(key, part):
    devices_all = VERTS // V_DEV
    half = IFD // 2
    flip_dev, cols_up, rows_up, source_down, group_of, member_of, tile_key, fill_key = dom_plan(key)
    upward = tile_noise(tile_key, (devices_all, half, TILE, TILE))
    slot_ids = jnp.arange(half, dtype=jnp.int32)[None, :]
    downward = jnp.swapaxes(upward[source_down, slot_ids], 2, 3)
    return jnp.concatenate([upward, downward], axis=1).reshape(devices_all * IFD, TILE, TILE)


def draw_dom_cols(key, part):
    half = IFD // 2
    flip_dev, cols_up, rows_up, source_down, group_of, member_of, tile_key, fill_key = dom_plan(key)
    slot_ids = jnp.arange(half, dtype=jnp.int32)[None, :]
    return jnp.concatenate([cols_up, rows_up[source_down, slot_ids]], axis=1).reshape(-1).astype(jnp.int32)


def draw_dom_slots(key, part):
    half = IFD // 2
    flip_dev, cols_up, rows_up, source_down, group_of, member_of, tile_key, fill_key = dom_plan(key)
    slot_ids = jnp.arange(half, dtype=jnp.int32)[None, :]
    partner = jnp.bitwise_xor(group_of[:, None], flip_dev)
    upward = partner * SD + slot_ids
    downward = partner * SD + half + slot_ids
    return jnp.concatenate([upward, downward], axis=1).reshape(-1).astype(jnp.int32)


def draw_dom_rows(key, part):
    devices_all = VERTS // V_DEV
    half = IFD // 2
    flip_dev, cols_up, rows_up, source_down, group_of, member_of, tile_key, fill_key = dom_plan(key)
    filler = jax.random.randint(fill_key, (devices_all, N_DOM, SD), 0, NB, dtype=jnp.int32)
    groups = jnp.arange(N_DOM, dtype=jnp.int32)[None, :, None]
    mine = group_of[:, None, None]
    flip_full = jnp.concatenate([flip_dev, flip_dev], axis=1)[:, None, :]
    slots = jnp.arange(SD, dtype=jnp.int32)[None, None, :]
    is_down = slots >= half
    slot_mod = slots % half
    matched = jnp.bitwise_xor(groups, flip_full) == mine
    sender = groups * N_SUB + member_of[:, None, None]
    up_value = rows_up[sender, slot_mod]
    own = jnp.arange(devices_all, dtype=jnp.int32)[:, None, None]
    down_value = cols_up[own, slot_mod]
    result = jnp.where(matched, jnp.where(is_down, down_value, up_value), filler)
    return result.reshape(-1).astype(jnp.int32)


def sub_plan(key):
    devices_all = VERTS // V_DEV
    half = IFS // 2
    subkeys = jax.random.split(jax.random.fold_in(key, 23), 5)
    turn = jax.random.randint(subkeys[0], (N_DOM,), 0, N_SUB - 1, dtype=jnp.int32)
    cols_up = jax.random.randint(subkeys[1], (devices_all, half), 0, NB, dtype=jnp.int32)
    rows_up = jax.random.randint(subkeys[2], (devices_all, half), 0, NB, dtype=jnp.int32)
    device_ids = jnp.arange(devices_all, dtype=jnp.int32)
    group_of = device_ids // N_SUB
    member_of = device_ids % N_SUB
    slot_ids = jnp.arange(half, dtype=jnp.int32)[None, :]
    offset_dev = 1 + (slot_ids + turn[group_of][:, None]) % (N_SUB - 1)
    level = slot_ids // (N_SUB - 1)
    source_down = group_of[:, None] * N_SUB + (member_of[:, None] - offset_dev) % N_SUB
    return (turn, cols_up, rows_up, offset_dev, level, source_down, group_of, member_of, subkeys[3], subkeys[4])


def draw_sub_tiles(key, part):
    devices_all = VERTS // V_DEV
    half = IFS // 2
    turn, cols_up, rows_up, offset_dev, level, source_down, group_of, member_of, tile_key, fill_key = sub_plan(key)
    upward = tile_noise(tile_key, (devices_all, half, TILE, TILE))
    slot_ids = jnp.arange(half, dtype=jnp.int32)[None, :]
    downward = jnp.swapaxes(upward[source_down, slot_ids], 2, 3)
    return jnp.concatenate([upward, downward], axis=1).reshape(devices_all * IFS, TILE, TILE)


def draw_sub_cols(key, part):
    half = IFS // 2
    turn, cols_up, rows_up, offset_dev, level, source_down, group_of, member_of, tile_key, fill_key = sub_plan(key)
    slot_ids = jnp.arange(half, dtype=jnp.int32)[None, :]
    return jnp.concatenate([cols_up, rows_up[source_down, slot_ids]], axis=1).reshape(-1).astype(jnp.int32)


def draw_sub_slots(key, part):
    turn, cols_up, rows_up, offset_dev, level, source_down, group_of, member_of, tile_key, fill_key = sub_plan(key)
    upward = (member_of[:, None] + offset_dev) % N_SUB * SS + level
    downward = (member_of[:, None] - offset_dev) % N_SUB * SS + SS // 2 + level
    return jnp.concatenate([upward, downward], axis=1).reshape(-1).astype(jnp.int32)


def draw_sub_rows(key, part):
    devices_all = VERTS // V_DEV
    half = IFS // 2
    half_slots = SS // 2
    turn, cols_up, rows_up, offset_dev, level, source_down, group_of, member_of, tile_key, fill_key = sub_plan(key)
    filler = jax.random.randint(fill_key, (devices_all, N_SUB, SS), 0, NB, dtype=jnp.int32)
    others = jnp.arange(N_SUB, dtype=jnp.int32)[None, :, None]
    mine = member_of[:, None, None]
    group_here = group_of[:, None, None]
    slots = jnp.arange(SS, dtype=jnp.int32)[None, None, :]
    is_down = slots >= half_slots
    depth = jnp.where(is_down, slots - half_slots, slots)
    needed = jnp.where(is_down, (others - mine) % N_SUB, (mine - others) % N_SUB)
    rest = (needed - 1 - turn[group_of][:, None, None]) % (N_SUB - 1)
    index = depth * (N_SUB - 1) + rest
    valid = (needed != 0) & (index < half)
    safe = jnp.clip(index, 0, half - 1)
    sender = group_here * N_SUB + others
    up_value = rows_up[sender, safe]
    own = jnp.broadcast_to(jnp.arange(devices_all, dtype=jnp.int32)[:, None, None], (devices_all, N_SUB, SS))
    down_value = cols_up[own, safe]
    chosen = jnp.where(is_down, down_value, up_value)
    return jnp.where(valid, chosen, filler).reshape(-1).astype(jnp.int32)


def draw_precond(key, part):
    total = VERTS // TILE
    first, second = jax.random.split(key)
    noise = jax.random.normal(first, (total, TILE, TILE), jnp.float32) * (0.045 / math.sqrt(TILE))
    noise = jnp.clip((noise + jnp.swapaxes(noise, 1, 2)) * 0.7071, -0.05, 0.05)
    diagonal = jax.random.uniform(second, (total, TILE), jnp.float32, 0.12, 0.3)
    identity_tile = jnp.eye(TILE, dtype=jnp.float32)
    return noise * (1.0 - identity_tile) + identity_tile * diagonal[:, :, None]


def shard_levels(rng, dims, shards, smallest, largest):
    level, own = 1.0, jax.random.fold_in(rng, 6)
    for dim, blocks in shards:
        steps = jnp.exp(jax.random.uniform(jax.random.fold_in(own, dim), (blocks,), jnp.float32, smallest / len(shards), largest / len(shards)))
        level = level * jnp.repeat(steps, dims[dim] // blocks).reshape([-1 if axis == dim else 1 for axis in range(len(dims))])
    return level


def setup_inputs(seed: int = 0) -> dict:
    streams_of = jax.random.split(jax.random.key(seed), 16)
    return {
        "positions": draw_positions(jax.random.fold_in(streams_of[15], 71), 0),
        "mass": jnp.clip(3.0 + 3.0 * jax.random.uniform(streams_of[1], (VERTS,), jnp.float32) ** shard_levels(streams_of[1], (VERTS,), ((0, 32),), -0.2, 0.2), 3.0, 6.0),
        "local_tiles": draw_local_tiles(jax.random.fold_in(streams_of[15], 71), 0),
        "local_rows": draw_local_rows(jax.random.fold_in(streams_of[15], 71), 0),
        "local_cols": draw_local_cols(jax.random.fold_in(streams_of[15], 71), 0),
        "live_tiles": draw_live_tiles(jax.random.fold_in(streams_of[15], 71), 0),
        "dom_tiles": draw_dom_tiles(jax.random.fold_in(streams_of[15], 71), 0),
        "dom_cols": draw_dom_cols(jax.random.fold_in(streams_of[15], 71), 0),
        "dom_slots": draw_dom_slots(jax.random.fold_in(streams_of[15], 71), 0),
        "dom_rows": draw_dom_rows(jax.random.fold_in(streams_of[15], 71), 0),
        "sub_tiles": draw_sub_tiles(jax.random.fold_in(streams_of[15], 71), 0),
        "sub_cols": draw_sub_cols(jax.random.fold_in(streams_of[15], 71), 0),
        "sub_slots": draw_sub_slots(jax.random.fold_in(streams_of[15], 71), 0),
        "sub_rows": draw_sub_rows(jax.random.fold_in(streams_of[15], 71), 0),
        "precond": draw_precond(jax.random.fold_in(streams_of[15], 71), 0),
    }


PRECISE = lax.Precision.HIGHEST


def tile_terms(tile_stack, columns, blocks, devices_all):
    per_device = tile_stack.shape[0] // devices_all
    owners = jnp.arange(tile_stack.shape[0], dtype=jnp.int32) // per_device
    picked = jnp.take(blocks, owners * NB + columns, axis=1)
    products = jnp.einsum("tij,ktj->tki", tile_stack, picked, precision=PRECISE)
    return products, owners, per_device


def apply_operator(vector, mass, local_tiles, local_rows, local_cols, live_tiles, dom_tiles, dom_cols, dom_slots, dom_rows, sub_tiles, sub_cols, sub_slots, sub_rows):
    devices_all = VERTS // V_DEV
    components = vector.shape[0]
    blocks = vector.reshape(components, devices_all * NB, TILE)
    products, owners, per_device = tile_terms(local_tiles, local_cols, blocks, devices_all)
    place_in = jnp.arange(local_tiles.shape[0], dtype=jnp.int32) - owners * per_device
    live_mask = (place_in < live_tiles[owners]).astype(vector.dtype)
    summed = jax.ops.segment_sum(products * live_mask[:, None, None], owners * NB + local_rows, num_segments=devices_all * NB)
    products, owners, per_device = tile_terms(dom_tiles, dom_cols, blocks, devices_all)
    outgoing = jax.ops.segment_sum(products, owners * (N_DOM * SD) + dom_slots, num_segments=devices_all * N_DOM * SD)
    outgoing = outgoing.reshape(N_DOM, N_SUB, N_DOM, SD, components, TILE).transpose(2, 1, 0, 3, 4, 5)
    outgoing = outgoing.reshape(devices_all * N_DOM * SD, components, TILE)
    receivers = jnp.arange(devices_all * N_DOM * SD, dtype=jnp.int32) // (N_DOM * SD)
    summed = summed + jax.ops.segment_sum(outgoing, receivers * NB + dom_rows, num_segments=devices_all * NB)
    products, owners, per_device = tile_terms(sub_tiles, sub_cols, blocks, devices_all)
    outgoing = jax.ops.segment_sum(products, owners * (N_SUB * SS) + sub_slots, num_segments=devices_all * N_SUB * SS)
    outgoing = outgoing.reshape(N_DOM, N_SUB, N_SUB, SS, components, TILE).transpose(0, 2, 1, 3, 4, 5)
    outgoing = outgoing.reshape(devices_all * N_SUB * SS, components, TILE)
    receivers = jnp.arange(devices_all * N_SUB * SS, dtype=jnp.int32) // (N_SUB * SS)
    summed = summed + jax.ops.segment_sum(outgoing, receivers * NB + sub_rows, num_segments=devices_all * NB)
    return mass[None, :] * vector + summed.transpose(1, 0, 2).reshape(components, VERTS)


def apply_precond(vector, precond):
    components = vector.shape[0]
    blocks = vector.reshape(components, VERTS // TILE, TILE)
    return jnp.einsum("bij,kbj->kbi", precond, blocks, precision=PRECISE).reshape(components, VERTS)


def reference(positions, mass, local_tiles, local_rows, local_cols, live_tiles, dom_tiles, dom_cols, dom_slots, dom_rows, sub_tiles, sub_cols, sub_slots, sub_rows, precond):
    def operate(vector):
        return apply_operator(vector, mass, local_tiles, local_rows, local_cols, live_tiles, dom_tiles, dom_cols, dom_slots, dom_rows, sub_tiles, sub_cols, sub_slots, sub_rows)

    solution = positions
    residual = mass[None, :] * positions - operate(positions)
    smoothed = apply_precond(residual, precond)
    direction = smoothed
    current = jnp.sum(residual * smoothed, axis=1)
    for iteration in range(ITERS):
        applied = operate(direction)
        step_size = current / jnp.sum(direction * applied, axis=1)
        solution = solution + step_size[:, None] * direction
        residual = residual - step_size[:, None] * applied
        if iteration + 1 < ITERS:
            smoothed = apply_precond(residual, precond)
            following = jnp.sum(residual * smoothed, axis=1)
            direction = smoothed + (following / current)[:, None] * direction
            current = following
    return solution, residual
```

```python
import functools

import jax
import jax.numpy as jnp
from jax import lax
from jax.experimental import pallas as pl
from jax.experimental.pallas import tpu as pltpu
from jax.sharding import PartitionSpec as P

ITERS = 3
SHIFT = 1.0
CHUNK = 16
F32 = jnp.float32
BF16 = jnp.bfloat16
MESH = pl.DeviceIdType.MESH


def high(value):
    return value.astype(BF16).astype(F32)


def kernel(count_dom, count_sub, bits, pos_hbm, mass_hbm, local_rows_hbm, live_hbm, dom_rows_hbm, dom_slots_hbm,
           sub_rows_hbm, sub_slots_hbm, dom_cols_flat, local_cols_hbm, dom_cols_hbm, sub_cols_hbm, local_hbm, dom_hbm, sub_hbm, pre_hbm, sol_hbm, res_hbm,
           stage, weights, place, vec, image, expanded, products, local_rows, live, dom_rows, dom_slots, sub_rows,
           sub_slots, dom_cols_s, send_dom, recv_dom, send_sub, recv_sub,
           sums, own, load_sem, dom_send_sem, dom_recv_sem, sub_send_sem, sub_recv_sem,
           red_send, red_recv, pos_ref, mass_ref, local_cols, dom_cols, sub_cols, sol_ref, res_ref,
           small_sem, far_sem):
    lt, ld, ls, nb = local_hbm.shape[0], dom_hbm.shape[0], sub_hbm.shape[0], pre_hbm.shape[0]
    tile = pre_hbm.shape[1]
    width_dom = dom_rows_hbm.shape[0] // count_dom
    width_sub = sub_rows_hbm.shape[0] // count_sub
    a = lax.axis_index("dom")
    b = lax.axis_index("sub")
    tiles = lt + ld + ls

    def partner_dom(j):
        bit = 1 << j
        return a + bit - 2 * bit * ((a // bit) % 2)

    small = []
    for source, target in ((pos_hbm, pos_ref), (dom_rows_hbm, dom_rows), (sub_rows_hbm, sub_rows),
                           (local_cols_hbm, local_cols), (dom_cols_hbm, dom_cols), (sub_cols_hbm, sub_cols),
                           (local_rows_hbm, local_rows), (live_hbm, live), (sub_slots_hbm, sub_slots),
                           (dom_slots_hbm, dom_slots), (mass_hbm, mass_ref), (dom_cols_flat, dom_cols_s)):
        copy = pltpu.make_async_copy(source, target, small_sem.at[len(small)])
        copy.start()
        small.append(copy)

    barrier = pltpu.get_barrier_semaphore()
    for j in range(bits):
        pl.semaphore_signal(barrier, inc=1, device_id=(partner_dom(j), b), device_id_type=MESH)
    for o in range(1, count_sub):
        pl.semaphore_signal(barrier, inc=1, device_id=(a, (b + o) % count_sub), device_id_type=MESH)

    loads = {}
    for start, source in ((0, local_hbm), (tiles, pre_hbm), (lt + ld, sub_hbm), (lt, dom_hbm)):
        for first in range(0, source.shape[0], CHUNK):
            copy = pltpu.make_async_copy(source.at[pl.ds(first, CHUNK)], stage.at[pl.ds(start + first, CHUNK)],
                                         load_sem.at[(start + first) // CHUNK])
            copy.start()
            loads[(start + first) // CHUNK] = copy

    sub8 = lax.broadcasted_iota(jnp.int32, (8, tile), 0)
    upper = sub8 < 4
    zero1 = jnp.zeros((1, tile), F32)

    def doubled(three):
        return jnp.concatenate([three, zero1, three, zero1], axis=0)

    def split_rows(value):
        h = high(value)
        return jnp.where(upper, h, value - h)

    with jax.named_scope('small_wait'):
        for copy in small[:3]:
            copy.wait()

    for k in range(nb):
        vec[0, k] = doubled(pos_ref[:, k * tile:(k + 1) * tile])

    def exchange(k):
        copies = []
        for j in reversed(range(bits)):
            other = partner_dom(j)
            for s in range(width_dom):
                send_dom[k, j, 3 * s:3 * s + 3, :] = vec[k, dom_rows[other * width_dom + s], 0:3, :]
            copy = pltpu.make_async_remote_copy(
                src_ref=send_dom.at[k, j], dst_ref=recv_dom.at[k, j], send_sem=dom_send_sem.at[k, j],
                recv_sem=dom_recv_sem.at[k, j], device_id=(other, b), device_id_type=MESH)
            copy.start()
            copies.append(copy)
        for o in range(1, count_sub):
            other = (b + o) % count_sub
            for s in range(width_sub):
                send_sub[k, o - 1, 3 * s:3 * s + 3, :] = vec[k, sub_rows[other * width_sub + s], 0:3, :]
            copy = pltpu.make_async_remote_copy(
                src_ref=send_sub.at[k, o - 1], dst_ref=recv_sub.at[k, o - 1], send_sem=sub_send_sem.at[k, o - 1],
                recv_sem=sub_recv_sem.at[k, o - 1], device_id=(a, other), device_id_type=MESH)
            copy.start()
            copies.append(copy)
        return copies

    def expand_own(k):
        for n in range(nb):
            expanded[n] = split_rows(vec[k, n])

    def expand_received(k, copies):
        for o in range(1, count_sub):
            copies[bits + o - 1].wait_recv()
            base = nb + count_dom * width_dom + ((b + count_sub - o) % count_sub) * width_sub
            for s in range(width_sub):
                expanded[base + s] = split_rows(doubled(recv_sub[k, o - 1, 3 * s:3 * s + 3, :]))

    def expand_received_dom(k, copies):
        for j in rounds[k]:
            pl.semaphore_wait(far_sem.at[j], 1)
        for j in range(bits):
            copies[bits - 1 - j].wait_recv()
            base = nb + partner_dom(j) * width_dom
            for s in range(width_dom):
                expanded[base + s] = split_rows(doubled(recv_dom[k, j, 3 * s:3 * s + 3, :]))

    def multiply(left, right, pair):
        rows = jnp.concatenate([left, right], axis=0).astype(BF16)
        out = jnp.dot(jnp.concatenate([rows, rows], axis=1), weights[pair], preferred_element_type=F32)
        return out[0:8, 0:tile], out[8:16, tile:2 * tile]

    def block_of(t, base):
        if base == "local":
            return local_rows[t]
        if base == "dom":
            return nb + dom_slots[t - lt]
        return nb + count_dom * width_dom + sub_slots[t - lt - ld]

    def one_pair(p, base):
        left, right = multiply(expanded[block_of(2 * p, base)], expanded[block_of(2 * p + 1, base)], p)
        both = jnp.concatenate([left, right], axis=0)
        h = both.astype(BF16)
        low = (both - h.astype(F32)).astype(BF16)
        products[pl.ds(pl.multiple_of(16 * p, 16), 16), :] = jnp.concatenate([h, low], axis=1)
        return left, right

    def run_pairs(first, last, base):
        unroll = last - first if last - first <= 24 else 16
        def body(i, carry):
            for u in range(unroll):
                one_pair(first + i * unroll + u, base)
            return carry
        lax.fori_loop(0, (last - first) // unroll, body, 0)

    def scatter(first, last):
        out = jnp.dot(place[:, 8 * first:8 * last], products[8 * first:8 * last, :], preferred_element_type=F32)
        return (out[:, 0:tile] + out[:, tile:2 * tile]).reshape(nb, 8, tile)

    def apply_pre(k):
        for p in range(nb // 2):
            left, right = multiply(split_rows(image[k, 2 * p]), split_rows(image[k, 2 * p + 1]), tiles // 2 + p)
            left = left + pltpu.roll(left, 4, 0)
            right = right + pltpu.roll(right, 4, 0)
            if k > 0:
                left = left - SHIFT * vec[k, 2 * p]
                right = right - SHIFT * vec[k, 2 * p + 1]
            vec[k + 1, 2 * p] = left
            vec[k + 1, 2 * p + 1] = right

    with jax.named_scope('small_wait2'):
        expand_own(0)
        for copy in small[3:]:
            copy.wait()

    column = 0
    for cols in (local_cols, dom_cols, sub_cols):
        n = cols.shape[1]
        reach = (lax.broadcasted_iota(jnp.int32, (n, 8 * n), 1) // 8
                 == lax.broadcasted_iota(jnp.int32, (n, 8 * n), 0)).astype(F32).astype(BF16)
        spread = jnp.dot(jnp.broadcast_to(cols[...].astype(F32), (8, n)).astype(BF16), reach,
                         preferred_element_type=F32)
        pattern = ((lax.broadcasted_iota(jnp.int32, (8, 8 * n), 1) % 4)
                   == (lax.broadcasted_iota(jnp.int32, (8, 8 * n), 0) % 4))
        spread = jnp.where(pattern, spread, -1.0)
        for k in range(0, nb, 2):
            low = jnp.where(jnp.abs(spread - k) < 0.5, 1.0, 0.0)
            up = jnp.where(jnp.abs(spread - (k + 1)) < 0.5, 1.0, 0.0)
            place[8 * k:8 * k + 16, column:column + 8 * n] = jnp.concatenate([low, up], axis=0).astype(BF16)
        column += 8 * n

    with jax.named_scope('barrier'):
        pl.semaphore_wait(barrier, bits + count_sub - 1)
    with jax.named_scope('exch#k=0'):
        copies = [exchange(0)]
    used = live[0]

    def convert(p, masked):
        for side in range(2):
            value = stage[2 * p + side]
            if masked:
                value = value * (2 * p + side < used).astype(F32)
            h = value.astype(BF16)
            weights[p, 0:tile, side * tile:(side + 1) * tile] = h
            weights[p, tile:2 * tile, side * tile:(side + 1) * tile] = (value - h.astype(F32)).astype(BF16)

    def arrive(first, last, masked=False, multiplied=False, unroll=4):
        for c in range(first // CHUNK, last // CHUNK):
            loads[c].wait()

            def body(i, carry):
                for u in range(unroll):
                    convert(c * CHUNK // 2 + i * unroll + u, masked)
                if multiplied:
                    for u in range(unroll):
                        one_pair(c * CHUNK // 2 + i * unroll + u, "local")
                return carry
            lax.fori_loop(0, CHUNK // 2 // unroll, body, 0)

    pairs = [(i, j) for i in range(ITERS) for j in range(i, ITERS)]

    def inner(sums):
        totals = [jnp.zeros((8, tile), F32)] * len(sums)
        for n in range(nb):
            vectors = {i: vec[i + 1, n] for i in {x for x, _ in sums}}
            images = {j: image[j, n] for j in {y for _, y in sums}}
            totals = [t + vectors[x] * images[y] for t, (x, y) in zip(totals, sums)]
        return totals

    row_of = sub8 % 4
    lane = lax.broadcasted_iota(jnp.int32, (8, tile), 1)
    span = tile // 4
    last = ITERS - 1
    order = [(i, 0) for i in range(ITERS)] + [(j, i + 1) for i, j in pairs if i < last]
    reductions = []

    def share(which, packed):
        own[which] = jnp.sum(packed, axis=0, keepdims=True)
        group = []
        for o in reversed(range(1, count_dom * count_sub)):
            target = ((a + o // count_sub) % count_dom, (b + o % count_sub) % count_sub)
            copy = pltpu.make_async_remote_copy(
                src_ref=own.at[which], dst_ref=sums.at[which, o - 1], send_sem=red_send.at[which, o - 1],
                recv_sem=red_recv.at[which, o - 1], device_id=target, device_id_type=MESH)
            copy.start()
            group.append(copy)
        reductions.append(group)

    def shared(which):
        for copy in reductions[which]:
            copy.wait_recv()
        parts = [own[which]] + [sums[which, o] for o in range(count_dom * count_sub - 1)]
        while len(parts) > 1:
            parts = [x + y for x, y in zip(parts[::2], parts[1::2])] + (parts[-1:] if len(parts) % 2 else [])
        return jnp.broadcast_to(parts[0], (8, tile))

    def pick(row, i):
        mine = jnp.where(lane == span * row_of + i, row, 0.0)
        return jnp.sum(mine, axis=1, keepdims=True) + jnp.zeros((8, tile), F32)

    rounds = [range(0, 0)] + [range((k - 1) * bits // ITERS, k * bits // ITERS) for k in range(1, ITERS + 1)]
    for k in range(ITERS + 1):
        if k > 0:
            with jax.named_scope(f'exch#k={k}'):
                copies.append(exchange(k))
                for j in rounds[k]:
                    pl.semaphore_signal(far_sem.at[j], inc=1, device_id=(partner_dom(j), b), device_id_type=MESH)
            with jax.named_scope(f'own#k={k}'):
                expand_own(k)
                run_pairs(0, lt // 2, "local")
        else:
            with jax.named_scope('arrive_local'):
                arrive(0, lt, True)
                run_pairs(0, lt // 2, "local")
        part = scatter(0, lt)
        for n in range(nb):
            if k > 0:
                image[k, n] = part[n] + mass_ref[n:n + 1, :] * vec[k, n]
            else:
                image[k, n] = part[n]
        if k == ITERS:
            packed = jnp.zeros((8, tile), F32)
            for i, total in enumerate(inner(order)):
                value = jnp.sum(total, axis=1, keepdims=True)
                packed = jnp.where((lane == span * row_of + i) & (sub8 < 3), value, packed)
            share(0, packed)
        if k == 0:
            with jax.named_scope('arrive_rest'):
                arrive(tiles, tiles + nb)
                arrive(lt + ld, tiles)
                arrive(lt, lt + ld)
        with jax.named_scope(f'recvsub#k={k}'):
            expand_received(k, copies[k])
        with jax.named_scope(f'runsub#k={k}'):
            run_pairs((lt + ld) // 2, tiles // 2, "sub")
            part = scatter(lt + ld, tiles)
            for n in range(nb):
                image[k, n] = image[k, n] + part[n]
        if k == ITERS:
            late = jnp.where(upper, inner([(last, ITERS)])[0], 0.0)
        with jax.named_scope(f'recvdom#k={k}'):
            expand_received_dom(k, copies[k])
        with jax.named_scope(f'rundom#k={k}'):
            if k < ITERS:
                run_pairs(lt // 2, (lt + ld) // 2, "dom")
            else:
                for p in range(lt // 2, (lt + ld) // 2):
                    left, right = one_pair(p, "dom")
                    late = late + left * vec[k, dom_cols_s[2 * p - lt]] + right * vec[k, dom_cols_s[2 * p + 1 - lt]]
                value = jnp.sum(late, axis=1, keepdims=True)
                share(1, jnp.where((lane == span * row_of) & (row_of < 3), value, 0.0))
            part = scatter(lt, lt + ld)
            for n in range(nb):
                if k > 0:
                    image[k, n] = image[k, n] + part[n]
                else:
                    image[k, n] = -(image[k, n] + part[n])
        if k < ITERS:
            with jax.named_scope(f'pre#k={k}'):
                apply_pre(k)

    with jax.named_scope('red0_wait'):
        row = shared(0)
    gram = {}
    for i, pair in enumerate(order[ITERS:]):
        gram[pair[0], pair[1] - 1] = gram[pair[1] - 1, pair[0]] = pick(row, ITERS + i)
    first = [pick(row, i) for i in range(ITERS)]

    def add(x, y):
        return y if x is None else x if y is None else x + y

    direction = [jnp.ones((8, tile), F32)] + [None] * (ITERS - 1)
    coefs = [None] * ITERS
    current = first[0]
    for it in range(ITERS):
        used_terms = [i for i in range(ITERS) if direction[i] is not None]
        curvature = None
        for i in used_terms:
            inner_sum = None
            for j in used_terms:
                if (i, j) in gram:
                    inner_sum = add(inner_sum, gram[i, j] * direction[j])
            curvature = add(curvature, direction[i] * inner_sum)
        if it == last:
            break
        step = current / curvature
        for i in used_terms:
            coefs[i] = add(coefs[i], step * direction[i])
        if it + 1 < ITERS:
            smooth = [jnp.ones((8, tile), F32)] + [None] * (ITERS - 1)
            for j in range(it + 1):
                smooth[j + 1] = add(smooth[j + 1], -coefs[j])
                smooth[j] = add(smooth[j], -SHIFT * coefs[j])
            following = None
            for i in range(ITERS):
                if smooth[i] is None:
                    continue
                inner = first[i]
                for j in range(it + 1):
                    inner = inner - coefs[j] * gram[i, j]
                following = add(following, smooth[i] * inner)
            ratio = following / current
            direction = [add(s, None if d is None else ratio * d) for s, d in zip(smooth, direction)]
            current = following

    for n in range(nb):
        x, r, along, image_along = vec[0, n], image[0, n], None, None
        for i in range(ITERS):
            if coefs[i] is not None:
                x = x + coefs[i] * vec[i + 1, n]
                r = r - coefs[i] * image[i + 1, n]
            along = add(along, direction[i] * vec[i + 1, n])
            image_along = add(image_along, direction[i] * image[i + 1, n])
        vec[0, n], image[0, n], vec[1, n], image[1, n] = x, r, along, image_along

    with jax.named_scope('red1_wait'):
        row = shared(1)
    step = current / (curvature + direction[last] * direction[last] * pick(row, 0))
    for n in range(nb):
        x = vec[0, n] + step * vec[1, n]
        r = image[0, n] - step * image[1, n]
        sol_ref[:, n * tile:(n + 1) * tile] = x[0:3, :]
        res_ref[:, n * tile:(n + 1) * tile] = r[0:3, :]

    final = [pltpu.make_async_copy(sol_ref, sol_hbm, small_sem.at[0]),
             pltpu.make_async_copy(res_ref, res_hbm, small_sem.at[1])]
    for copy in final:
        copy.start()
    with jax.named_scope('final_wait'):
        for copy in final:
            copy.wait()

    with jax.named_scope('send_wait'):
        for group in copies:
            for copy in group:
                copy.wait_send()
    for group in reductions:
        for copy in group:
            copy.wait_send()


def finish(sol_in, res_in, sol_ref, res_ref):
    sol_ref[...] = sol_in[...]
    res_ref[...] = res_in[...]


def on_device(positions, mass, local_tiles, local_rows, local_cols, live_tiles, dom_tiles, dom_cols, dom_slots,
              dom_rows, sub_tiles, sub_cols, sub_slots, sub_rows, precond):
    count_dom = lax.axis_size("dom")
    count_sub = lax.axis_size("sub")
    bits = count_dom.bit_length() - 1
    nb, tile = precond.shape[0], precond.shape[1]
    lt, ld, ls = local_tiles.shape[0], dom_tiles.shape[0], sub_tiles.shape[0]
    tiles = lt + ld + ls
    width_dom = dom_rows.shape[0] // count_dom
    width_sub = sub_rows.shape[0] // count_sub
    vmem = pl.BlockSpec(memory_space=pltpu.VMEM)
    anym = pl.BlockSpec(memory_space=pltpu.HBM)
    k = ITERS + 1
    n_red = count_dom * count_sub - 1
    outs = pl.pallas_call(
        functools.partial(kernel, count_dom, count_sub, bits),
        out_shape=[jax.ShapeDtypeStruct(positions.shape, F32)] * 2,
        in_specs=[anym] * 16,
        out_specs=[anym, anym],
        scratch_shapes=[
            pltpu.VMEM((tiles + nb, tile, tile), F32),
            pltpu.VMEM(((tiles + nb) // 2, 2 * tile, 2 * tile), BF16),
            pltpu.VMEM((8 * nb, 8 * tiles), BF16),
            pltpu.VMEM((k, nb, 8, tile), F32),
            pltpu.VMEM((k, nb, 8, tile), F32),
            pltpu.VMEM((nb + count_dom * width_dom + count_sub * width_sub, 8, tile), F32),
            pltpu.VMEM((8 * tiles, 2 * tile), BF16),
            pltpu.SMEM(local_rows.shape, jnp.int32),
            pltpu.SMEM(live_tiles.shape, jnp.int32),
            pltpu.SMEM(dom_rows.shape, jnp.int32),
            pltpu.SMEM(dom_slots.shape, jnp.int32),
            pltpu.SMEM(sub_rows.shape, jnp.int32),
            pltpu.SMEM(sub_slots.shape, jnp.int32),
            pltpu.SMEM(dom_cols.shape, jnp.int32),
            pltpu.VMEM((k, bits, 3 * width_dom, tile), F32),
            pltpu.VMEM((k, bits, 3 * width_dom, tile), F32),
            pltpu.VMEM((k, count_sub - 1, 3 * width_sub, tile), F32),
            pltpu.VMEM((k, count_sub - 1, 3 * width_sub, tile), F32),
            pltpu.VMEM((2, count_dom * count_sub - 1, 1, tile), F32),
            pltpu.VMEM((2, 1, tile), F32),
            pltpu.SemaphoreType.DMA(((tiles + nb) // CHUNK,)),
            pltpu.SemaphoreType.DMA((k, bits)),
            pltpu.SemaphoreType.DMA((k, bits)),
            pltpu.SemaphoreType.DMA((k, count_sub - 1)),
            pltpu.SemaphoreType.DMA((k, count_sub - 1)),
            pltpu.SemaphoreType.DMA((2, n_red)),
            pltpu.SemaphoreType.DMA((2, n_red)),
            pltpu.VMEM(positions.shape, F32),
            pltpu.VMEM((nb, tile), F32),
            pltpu.VMEM((1, lt), jnp.int32),
            pltpu.VMEM((1, ld), jnp.int32),
            pltpu.VMEM((1, ls), jnp.int32),
            pltpu.VMEM(positions.shape, F32),
            pltpu.VMEM(positions.shape, F32),
            pltpu.SemaphoreType.DMA((12,)),
            pltpu.SemaphoreType.REGULAR((bits,)),
        ],
        compiler_params=pltpu.CompilerParams(
            collective_id=0, has_side_effects=True, vmem_limit_bytes=60 * 1024 * 1024),
        name="fairing",
    )(positions, mass.reshape(nb, tile), local_rows, live_tiles, dom_rows, dom_slots, sub_rows, sub_slots, dom_cols,
      local_cols.reshape(1, lt), dom_cols.reshape(1, ld), sub_cols.reshape(1, ls),
      local_tiles, dom_tiles, sub_tiles, precond)
    return pl.pallas_call(
        finish,
        out_shape=[jax.ShapeDtypeStruct(positions.shape, F32)] * 2,
        in_specs=[vmem, vmem],
        out_specs=[vmem, vmem],
        name="finish",
    )(*outs)


def solution(mesh):
    split = P(("dom", "sub"))
    tiled = P(("dom", "sub"), None, None)
    placed = (P(None, ("dom", "sub")), split, tiled, split, split, split, tiled, split, split, split, tiled, split,
              split, split, tiled)
    return jax.shard_map(
        on_device,
        mesh=mesh,
        in_specs=placed,
        out_specs=(P(None, ("dom", "sub")), P(None, ("dom", "sub"))),
        check_vma=False,
    )
```

```python
import functools

import jax
import jax.numpy as jnp
from jax import lax
from jax.experimental import pallas as pl
from jax.experimental.pallas import tpu as pltpu
from jax.sharding import PartitionSpec as P

ITERS = 3
SHIFT = 1.0
CHUNK = 16
F32 = jnp.float32
BF16 = jnp.bfloat16
MESH = pl.DeviceIdType.MESH


def high(value):
    return value.astype(BF16).astype(F32)


def drain(ref, sem):
    pltpu.make_async_copy(ref, ref, sem).wait()


def kernel(count_dom, count_sub, bits, pos_hbm, mass_hbm, local_rows_hbm, live_hbm, dom_rows_hbm, dom_slots_hbm,
           sub_rows_hbm, sub_slots_hbm, dom_cols_flat, local_cols_hbm, dom_cols_hbm, sub_cols_hbm, local_hbm, dom_hbm, sub_hbm, pre_hbm, sol_ref, res_ref,
           stage, weights, place, vec, image, expanded, products, local_rows, live, dom_rows, dom_slots, sub_rows,
           sub_slots, dom_cols_s, send_dom, recv_dom, send_sub, recv_sub,
           sums, own, load_sem, dom_send_sem, dom_recv_sem, sub_send_sem, sub_recv_sem,
           red_send, red_recv, pos_ref, mass_ref, local_cols, dom_cols, sub_cols,
           small_sem, far_sem):
    lt, ld, ls, nb = local_hbm.shape[0], dom_hbm.shape[0], sub_hbm.shape[0], pre_hbm.shape[0]
    tile = pre_hbm.shape[1]
    width_dom = dom_rows_hbm.shape[0] // count_dom
    width_sub = sub_rows_hbm.shape[0] // count_sub
    a = lax.axis_index("dom")
    b = lax.axis_index("sub")
    tiles = lt + ld + ls

    def partner_dom(j):
        bit = 1 << j
        return a + bit - 2 * bit * ((a // bit) % 2)

    small = []
    for source, target in ((pos_hbm, pos_ref), (dom_rows_hbm, dom_rows), (sub_rows_hbm, sub_rows),
                           (local_cols_hbm, local_cols), (dom_cols_hbm, dom_cols), (sub_cols_hbm, sub_cols),
                           (local_rows_hbm, local_rows), (live_hbm, live), (sub_slots_hbm, sub_slots),
                           (dom_slots_hbm, dom_slots), (mass_hbm, mass_ref), (dom_cols_flat, dom_cols_s)):
        copy = pltpu.make_async_copy(source, target, small_sem.at[min(len(small), 3)])
        copy.start()
        small.append(copy)

    barrier = pltpu.get_barrier_semaphore()
    for j in range(bits):
        pl.semaphore_signal(barrier, inc=1, device_id=(partner_dom(j), b), device_id_type=MESH)
    for o in range(1, count_sub):
        pl.semaphore_signal(barrier, inc=1, device_id=(a, (b + o) % count_sub), device_id_type=MESH)

    groups = ((0, 2 * CHUNK), (2 * CHUNK, lt), (lt + ld, tiles), (lt, lt + ld), (tiles, tiles + nb))
    sources = (local_hbm, local_hbm, sub_hbm, dom_hbm, pre_hbm)
    for g, ((first, end), source) in enumerate(zip(groups, sources)):
        offset = first if g < 2 else 0
        for c in range(0, end - first, CHUNK):
            pltpu.make_async_copy(source.at[pl.ds(offset + c, CHUNK)], stage.at[pl.ds(first + c, CHUNK)],
                                  load_sem.at[g]).start()

    def loaded(g):
        first, end = groups[g]
        drain(stage.at[pl.ds(first, end - first)], load_sem.at[g])

    sub8 = lax.broadcasted_iota(jnp.int32, (8, tile), 0)
    upper = sub8 < 4
    zero1 = jnp.zeros((1, tile), F32)

    def doubled(three):
        return jnp.concatenate([three, zero1, three, zero1], axis=0)

    def split_rows(value):
        h = high(value)
        return jnp.where(upper, h, value - h)

    with jax.named_scope('small_wait'):
        for copy in small[:3]:
            copy.wait()

    for k in range(nb):
        vec[0, k] = doubled(pos_ref[:, k * tile:(k + 1) * tile])

    def exchange(k):
        copies = {}
        for o in sorted(range(1, count_sub), key=lambda o: abs(2 * o - count_sub)):
            other = (b + o) % count_sub
            for s in range(width_sub):
                send_sub[k, o - 1, 3 * s:3 * s + 3, :] = vec[k, sub_rows[other * width_sub + s], 0:3, :]
            copy = pltpu.make_async_remote_copy(
                src_ref=send_sub.at[k, o - 1], dst_ref=recv_sub.at[k, o - 1], send_sem=sub_send_sem,
                recv_sem=sub_recv_sem.at[k % 2, o - 1], device_id=(a, other), device_id_type=MESH)
            copy.start()
            copies["sub", o] = copy
        for j in reversed(range(bits)):
            other = partner_dom(j)
            for s in range(width_dom):
                send_dom[k, j, 3 * s:3 * s + 3, :] = vec[k, dom_rows[other * width_dom + s], 0:3, :]
            copy = pltpu.make_async_remote_copy(
                src_ref=send_dom.at[k, j], dst_ref=recv_dom.at[k, j], send_sem=dom_send_sem,
                recv_sem=dom_recv_sem.at[k % 2, j], device_id=(other, b), device_id_type=MESH)
            copy.start()
            copies["dom", j] = copy
        return copies

    def expand_own(k):
        for n in range(nb):
            expanded[n] = split_rows(vec[k, n])

    def expand_received(k, copies):
        for o in range(1, count_sub):
            copies["sub", o].wait_recv()
            base = nb + count_dom * width_dom + ((b + count_sub - o) % count_sub) * width_sub
            for s in range(width_sub):
                expanded[base + s] = split_rows(doubled(recv_sub[k, o - 1, 3 * s:3 * s + 3, :]))

    def expand_received_dom(k, copies):
        for j in rounds[k]:
            pl.semaphore_wait(far_sem.at[j], 1)
        for j in range(bits):
            copies["dom", j].wait_recv()
            base = nb + partner_dom(j) * width_dom
            for s in range(width_dom):
                expanded[base + s] = split_rows(doubled(recv_dom[k, j, 3 * s:3 * s + 3, :]))

    def multiply(left, right, pair):
        rows = jnp.concatenate([left, right], axis=0).astype(BF16)
        out = jnp.dot(jnp.concatenate([rows, rows], axis=1), weights[pair], preferred_element_type=F32)
        return out[0:8, 0:tile], out[8:16, tile:2 * tile]

    def block_of(t, base):
        if base == "local":
            return local_rows[t]
        if base == "dom":
            return nb + dom_slots[t - lt]
        return nb + count_dom * width_dom + sub_slots[t - lt - ld]

    def one_pair(p, base):
        left, right = multiply(expanded[block_of(2 * p, base)], expanded[block_of(2 * p + 1, base)], p)
        both = jnp.concatenate([left, right], axis=0)
        h = both.astype(BF16)
        low = (both - h.astype(F32)).astype(BF16)
        products[pl.ds(pl.multiple_of(16 * p, 16), 16), :] = jnp.concatenate([h, low], axis=1)
        return left, right

    def run_pairs(first, last, base):
        for p in range(first, last):
            one_pair(p, base)

    def scatter(first, last):
        out = jnp.dot(place[:, 8 * first:8 * last], products[8 * first:8 * last, :], preferred_element_type=F32)
        return (out[:, 0:tile] + out[:, tile:2 * tile]).reshape(nb, 8, tile)

    def apply_pre(k):
        for p in range(nb // 2):
            left, right = multiply(split_rows(image[k, 2 * p]), split_rows(image[k, 2 * p + 1]), tiles // 2 + p)
            left = left + pltpu.roll(left, 4, 0)
            right = right + pltpu.roll(right, 4, 0)
            if k > 0:
                left = left - SHIFT * vec[k, 2 * p]
                right = right - SHIFT * vec[k, 2 * p + 1]
            vec[k + 1, 2 * p] = left
            vec[k + 1, 2 * p + 1] = right

    with jax.named_scope('small_wait2'):
        expand_own(0)
        for copy in small[3:]:
            copy.wait()

    column = 0
    for cols in (local_cols, dom_cols, sub_cols):
        n = cols.shape[1]
        reach = (lax.broadcasted_iota(jnp.int32, (n, 8 * n), 1) // 8
                 == lax.broadcasted_iota(jnp.int32, (n, 8 * n), 0)).astype(F32).astype(BF16)
        spread = jnp.dot(jnp.broadcast_to(cols[...].astype(F32), (8, n)).astype(BF16), reach,
                         preferred_element_type=F32)
        pattern = ((lax.broadcasted_iota(jnp.int32, (8, 8 * n), 1) % 4)
                   == (lax.broadcasted_iota(jnp.int32, (8, 8 * n), 0) % 4))
        spread = jnp.where(pattern, spread, -1.0)
        for k in range(0, nb, 2):
            low = jnp.where(jnp.abs(spread - k) < 0.5, 1.0, 0.0)
            up = jnp.where(jnp.abs(spread - (k + 1)) < 0.5, 1.0, 0.0)
            place[8 * k:8 * k + 16, column:column + 8 * n] = jnp.concatenate([low, up], axis=0).astype(BF16)
        column += 8 * n

    with jax.named_scope('barrier'):
        pl.semaphore_wait(barrier, bits + count_sub - 1)
    with jax.named_scope('exch#k=0'):
        copies = [exchange(0)]
    used = live[0]

    def convert(p, masked):
        for side in range(2):
            value = stage[2 * p + side]
            if masked:
                value = value * (2 * p + side < used).astype(F32)
            h = value.astype(BF16)
            weights[p, 0:tile, side * tile:(side + 1) * tile] = h
            weights[p, tile:2 * tile, side * tile:(side + 1) * tile] = (value - h.astype(F32)).astype(BF16)

    def convert_group(g, masked=False):
        first, end = groups[g]

        def body(i, carry):
            for u in range(8):
                convert(first // 2 + i * 8 + u, masked)
            return carry
        lax.fori_loop(0, (end - first) // 16, body, 0)

    pairs = [(i, j) for i in range(ITERS) for j in range(i, ITERS)]

    def inner(sums):
        totals = [jnp.zeros((8, tile), F32)] * len(sums)
        for n in range(nb):
            vectors = {i: vec[i + 1, n] for i in {x for x, _ in sums}}
            images = {j: image[j, n] for j in {y for _, y in sums}}
            totals = [t + vectors[x] * images[y] for t, (x, y) in zip(totals, sums)]
        return totals

    row_of = sub8 % 4
    lane = lax.broadcasted_iota(jnp.int32, (8, tile), 1)
    span = tile // 4
    last = ITERS - 1
    order = [(i, 0) for i in range(ITERS)] + [(j, i + 1) for i, j in pairs if i < last]

    def share(which, packed):
        own[which] = jnp.sum(packed, axis=0, keepdims=True)
        for o in reversed(range(1, count_dom * count_sub)):
            target = ((a + o // count_sub) % count_dom, (b + o % count_sub) % count_sub)
            copy = pltpu.make_async_remote_copy(
                src_ref=own.at[which], dst_ref=sums.at[which, o - 1], send_sem=red_send,
                recv_sem=red_recv.at[which], device_id=target, device_id_type=MESH)
            copy.start()

    def shared(which):
        drain(sums.at[which], red_recv.at[which])
        parts = [own[which]] + [sums[which, o] for o in range(count_dom * count_sub - 1)]
        while len(parts) > 1:
            parts = [x + y for x, y in zip(parts[::2], parts[1::2])] + (parts[-1:] if len(parts) % 2 else [])
        return jnp.broadcast_to(parts[0], (8, tile))

    def pick(row, i):
        mine = jnp.where(lane == span * row_of + i, row, 0.0)
        return jnp.sum(mine, axis=1, keepdims=True) + jnp.zeros((8, tile), F32)

    rounds = [range(0, 0)] + [range((k - 1) * bits // ITERS, k * bits // ITERS) for k in range(1, ITERS + 1)]
    for k in range(ITERS + 1):
        if k > 0:
            with jax.named_scope(f'exch#k={k}'):
                copies.append(exchange(k))
                for j in rounds[k]:
                    pl.semaphore_signal(far_sem.at[j], inc=1, device_id=(partner_dom(j), b), device_id_type=MESH)
            with jax.named_scope(f'own#k={k}'):
                expand_own(k)
                run_pairs(0, lt // 2, "local")
        else:
            with jax.named_scope('arrive_local'):
                loaded(0)
                convert_group(0, True)
                loaded(1)
                convert_group(1, True)
                loaded(2)
                run_pairs(0, lt // 2, "local")
                for p in range((lt + ld) // 2, tiles // 2):
                    convert(p, False)
        part = scatter(0, lt)
        for n in range(nb):
            if k > 0:
                image[k, n] = part[n] + mass_ref[n:n + 1, :] * vec[k, n]
            else:
                image[k, n] = part[n]
        if k == ITERS:
            packed = jnp.zeros((8, tile), F32)
            for i, total in enumerate(inner(order)):
                value = jnp.sum(total, axis=1, keepdims=True)
                packed = jnp.where((lane == span * row_of + i) & (sub8 < 3), value, packed)
            share(0, packed)
        if k == 0:
            with jax.named_scope('arrive_rest'):
                loaded(3)
                convert_group(3)
                loaded(4)
                convert_group(4)
        with jax.named_scope(f'recvsub#k={k}'):
            expand_received(k, copies[k])
        with jax.named_scope(f'runsub#k={k}'):
            run_pairs((lt + ld) // 2, tiles // 2, "sub")
            part = scatter(lt + ld, tiles)
            for n in range(nb):
                image[k, n] = image[k, n] + part[n]
        if k == ITERS:
            late = jnp.where(upper, inner([(last, ITERS)])[0], 0.0)
        with jax.named_scope(f'recvdom#k={k}'):
            expand_received_dom(k, copies[k])
        with jax.named_scope(f'rundom#k={k}'):
            if k < ITERS:
                run_pairs(lt // 2, (lt + ld) // 2, "dom")
            else:
                for p in range(lt // 2, (lt + ld) // 2):
                    left, right = one_pair(p, "dom")
                    late = late + left * vec[k, dom_cols_s[2 * p - lt]] + right * vec[k, dom_cols_s[2 * p + 1 - lt]]
                value = jnp.sum(late, axis=1, keepdims=True)
                share(1, jnp.where((lane == span * row_of) & (row_of < 3), value, 0.0))
            part = scatter(lt, lt + ld)
            for n in range(nb):
                if k > 0:
                    image[k, n] = image[k, n] + part[n]
                else:
                    image[k, n] = -(image[k, n] + part[n])
        if k < ITERS:
            with jax.named_scope(f'pre#k={k}'):
                apply_pre(k)

    with jax.named_scope('red0_wait'):
        row = shared(0)
    gram = {}
    for i, pair in enumerate(order[ITERS:]):
        gram[pair[0], pair[1] - 1] = gram[pair[1] - 1, pair[0]] = pick(row, ITERS + i)
    first = [pick(row, i) for i in range(ITERS)]

    def add(x, y):
        return y if x is None else x if y is None else x + y

    direction = [jnp.ones((8, tile), F32)] + [None] * (ITERS - 1)
    coefs = [None] * ITERS
    current = first[0]
    for it in range(ITERS):
        used_terms = [i for i in range(ITERS) if direction[i] is not None]
        curvature = None
        for i in used_terms:
            inner_sum = None
            for j in used_terms:
                if (i, j) in gram:
                    inner_sum = add(inner_sum, gram[i, j] * direction[j])
            curvature = add(curvature, direction[i] * inner_sum)
        if it == last:
            break
        step = current / curvature
        for i in used_terms:
            coefs[i] = add(coefs[i], step * direction[i])
        if it + 1 < ITERS:
            smooth = [jnp.ones((8, tile), F32)] + [None] * (ITERS - 1)
            for j in range(it + 1):
                smooth[j + 1] = add(smooth[j + 1], -coefs[j])
                smooth[j] = add(smooth[j], -SHIFT * coefs[j])
            following = None
            for i in range(ITERS):
                if smooth[i] is None:
                    continue
                inner = first[i]
                for j in range(it + 1):
                    inner = inner - coefs[j] * gram[i, j]
                following = add(following, smooth[i] * inner)
            ratio = following / current
            direction = [add(s, None if d is None else ratio * d) for s, d in zip(smooth, direction)]
            current = following

    for n in range(nb):
        x, r, along, image_along = vec[0, n], image[0, n], None, None
        for i in range(ITERS):
            if coefs[i] is not None:
                x = x + coefs[i] * vec[i + 1, n]
                r = r - coefs[i] * image[i + 1, n]
            along = add(along, direction[i] * vec[i + 1, n])
            image_along = add(image_along, direction[i] * image[i + 1, n])
        vec[0, n], image[0, n], vec[1, n], image[1, n] = x, r, along, image_along

    with jax.named_scope('red1_wait'):
        row = shared(1)
    step = current / (curvature + direction[last] * direction[last] * pick(row, 0))
    for n in range(nb):
        x = vec[0, n] + step * vec[1, n]
        r = image[0, n] - step * image[1, n]
        sol_ref[:, n * tile:(n + 1) * tile] = x[0:3, :]
        res_ref[:, n * tile:(n + 1) * tile] = r[0:3, :]

    with jax.named_scope('send_wait'):
        drain(send_sub, sub_send_sem)
        drain(send_dom, dom_send_sem)
        drain(sums, red_send)


def finish(sol_in, res_in, sol_ref, res_ref):
    sol_ref[...] = sol_in[...]
    res_ref[...] = res_in[...]


def on_device(positions, mass, local_tiles, local_rows, local_cols, live_tiles, dom_tiles, dom_cols, dom_slots,
              dom_rows, sub_tiles, sub_cols, sub_slots, sub_rows, precond):
    count_dom = lax.axis_size("dom")
    count_sub = lax.axis_size("sub")
    bits = count_dom.bit_length() - 1
    nb, tile = precond.shape[0], precond.shape[1]
    lt, ld, ls = local_tiles.shape[0], dom_tiles.shape[0], sub_tiles.shape[0]
    tiles = lt + ld + ls
    width_dom = dom_rows.shape[0] // count_dom
    width_sub = sub_rows.shape[0] // count_sub
    vmem = pl.BlockSpec(memory_space=pltpu.VMEM)
    anym = pl.BlockSpec(memory_space=pltpu.HBM)
    k = ITERS + 1
    n_red = count_dom * count_sub - 1
    outs = pl.pallas_call(
        functools.partial(kernel, count_dom, count_sub, bits),
        out_shape=[pltpu.VMEM(positions.shape, F32)] * 2,
        in_specs=[anym] * 16,
        out_specs=[vmem, vmem],
        scratch_shapes=[
            pltpu.VMEM((tiles + nb, tile, tile), F32),
            pltpu.VMEM(((tiles + nb) // 2, 2 * tile, 2 * tile), BF16),
            pltpu.VMEM((8 * nb, 8 * tiles), BF16),
            pltpu.VMEM((k, nb, 8, tile), F32),
            pltpu.VMEM((k, nb, 8, tile), F32),
            pltpu.VMEM((nb + count_dom * width_dom + count_sub * width_sub, 8, tile), F32),
            pltpu.VMEM((8 * tiles, 2 * tile), BF16),
            pltpu.SMEM(local_rows.shape, jnp.int32),
            pltpu.SMEM(live_tiles.shape, jnp.int32),
            pltpu.SMEM(dom_rows.shape, jnp.int32),
            pltpu.SMEM(dom_slots.shape, jnp.int32),
            pltpu.SMEM(sub_rows.shape, jnp.int32),
            pltpu.SMEM(sub_slots.shape, jnp.int32),
            pltpu.SMEM(dom_cols.shape, jnp.int32),
            pltpu.VMEM((k, bits, 3 * width_dom, tile), F32),
            pltpu.VMEM((k, bits, 3 * width_dom, tile), F32),
            pltpu.VMEM((k, count_sub - 1, 3 * width_sub, tile), F32),
            pltpu.VMEM((k, count_sub - 1, 3 * width_sub, tile), F32),
            pltpu.VMEM((2, count_dom * count_sub - 1, 1, tile), F32),
            pltpu.VMEM((2, 1, tile), F32),
            pltpu.SemaphoreType.DMA((5,)),
            pltpu.SemaphoreType.DMA,
            pltpu.SemaphoreType.DMA((2, bits)),
            pltpu.SemaphoreType.DMA,
            pltpu.SemaphoreType.DMA((2, count_sub - 1)),
            pltpu.SemaphoreType.DMA,
            pltpu.SemaphoreType.DMA((2,)),
            pltpu.VMEM(positions.shape, F32),
            pltpu.VMEM((nb, tile), F32),
            pltpu.VMEM((1, lt), jnp.int32),
            pltpu.VMEM((1, ld), jnp.int32),
            pltpu.VMEM((1, ls), jnp.int32),
            pltpu.SemaphoreType.DMA((4,)),
            pltpu.SemaphoreType.REGULAR((bits,)),
        ],
        compiler_params=pltpu.CompilerParams(
            collective_id=0, has_side_effects=True, vmem_limit_bytes=62914560),
        name="fairing",
    )(positions, mass.reshape(nb, tile), local_rows, live_tiles, dom_rows, dom_slots, sub_rows, sub_slots, dom_cols,
      local_cols.reshape(1, lt), dom_cols.reshape(1, ld), sub_cols.reshape(1, ls),
      local_tiles, dom_tiles, sub_tiles, precond)
    return pl.pallas_call(
        finish,
        out_shape=[jax.ShapeDtypeStruct(positions.shape, F32)] * 2,
        in_specs=[vmem, vmem],
        out_specs=[vmem, vmem],
        compiler_params=pltpu.CompilerParams(vmem_limit_bytes=8388608),
        name="finish",
    )(*outs)


def solution(mesh):
    split = P(("dom", "sub"))
    tiled = P(("dom", "sub"), None, None)
    placed = (P(None, ("dom", "sub")), split, tiled, split, split, split, tiled, split, split, split, tiled, split,
              split, split, tiled)
    return jax.shard_map(
        on_device,
        mesh=mesh,
        in_specs=placed,
        out_specs=(P(None, ("dom", "sub")), P(None, ("dom", "sub"))),
        check_vma=False,
    )
```

```python
import functools

import jax
import jax.numpy as jnp
from jax import lax
from jax.experimental import pallas as pl
from jax.experimental.pallas import tpu as pltpu
from jax.sharding import PartitionSpec as P

ITERS = 3
SHIFT = 1.0
CHUNK = 16
F32 = jnp.float32
BF16 = jnp.bfloat16
MESH = pl.DeviceIdType.MESH


def high(value):
    return value.astype(BF16).astype(F32)


def drain(ref, sem):
    pltpu.make_async_copy(ref, ref, sem).wait()


def kernel(count_dom, count_sub, bits, pos_hbm, mass_hbm, local_rows_hbm, live_hbm, dom_rows_hbm, dom_slots_hbm,
           sub_rows_hbm, sub_slots_hbm, dom_cols_flat, sub_cols_flat, local_cols_hbm, dom_cols_hbm, sub_cols_hbm, local_hbm, dom_hbm, sub_hbm, pre_hbm, sol_ref, res_ref,
           stage, weights, place, vec, image, expanded, products, local_rows, live, dom_rows, dom_slots, sub_rows,
           sub_slots, dom_cols_s, sub_cols_s, send_dom, recv_dom, send_sub, recv_sub,
           sums, own, load_sem, dom_send_sem, dom_recv_sem, sub_send_sem, sub_recv_sem,
           red_send, red_recv, pos_ref, mass_ref, local_cols, dom_cols, sub_cols,
           small_sem, far_sem, fused, blocks):
    lt, ld, ls, nb = local_hbm.shape[0], dom_hbm.shape[0], sub_hbm.shape[0], pre_hbm.shape[0]
    tile = pre_hbm.shape[1]
    width_dom = dom_rows_hbm.shape[0] // count_dom
    width_sub = sub_rows_hbm.shape[0] // count_sub
    a = lax.axis_index("dom")
    b = lax.axis_index("sub")
    tiles = lt + ld + ls

    def partner_dom(j):
        bit = 1 << j
        return a + bit - 2 * bit * ((a // bit) % 2)

    small = []
    for source, target in ((pos_hbm, pos_ref), (dom_rows_hbm, dom_rows), (sub_rows_hbm, sub_rows),
                           (local_cols_hbm, local_cols), (dom_cols_hbm, dom_cols), (sub_cols_hbm, sub_cols),
                           (local_rows_hbm, local_rows), (live_hbm, live), (sub_slots_hbm, sub_slots),
                           (dom_slots_hbm, dom_slots), (mass_hbm, mass_ref), (dom_cols_flat, dom_cols_s), (sub_cols_flat, sub_cols_s)):
        copy = pltpu.make_async_copy(source, target, small_sem.at[min(len(small), 3)])
        copy.start()
        small.append(copy)

    barrier = pltpu.get_barrier_semaphore()
    for j in reversed(range(bits)):
        pl.semaphore_signal(barrier, inc=1, device_id=(partner_dom(j), b), device_id_type=MESH)
    for o in range(1, count_sub):
        pl.semaphore_signal(barrier, inc=1, device_id=(a, (b + o) % count_sub), device_id_type=MESH)

    groups = ((0, 2 * CHUNK), (2 * CHUNK, lt), (lt + ld, tiles), (lt, lt + ld), (tiles, tiles + nb))
    sources = (local_hbm, local_hbm, sub_hbm, dom_hbm, pre_hbm)
    for g, ((first, end), source) in enumerate(zip(groups, sources)):
        offset = first if g < 2 else 0
        for c in range(0, end - first, CHUNK):
            pltpu.make_async_copy(source.at[pl.ds(offset + c, CHUNK)], stage.at[pl.ds(first + c, CHUNK)],
                                  load_sem.at[g]).start()

    def loaded(g):
        first, end = groups[g]
        drain(stage.at[pl.ds(first, end - first)], load_sem.at[g])

    sub8 = lax.broadcasted_iota(jnp.int32, (8, tile), 0)
    upper = sub8 < 4
    zero1 = jnp.zeros((1, tile), F32)

    def doubled(three):
        return jnp.concatenate([three, zero1, three, zero1], axis=0)

    def split_rows(value):
        h = high(value)
        return jnp.where(upper, h, value - h)

    with jax.named_scope('small_wait'):
        for copy in small[:3]:
            copy.wait()

    for k in range(nb):
        vec[0, k] = doubled(pos_ref[:, k * tile:(k + 1) * tile])

    def exchange(k):
        copies = {}
        for j in [bits - 1]:
            other = partner_dom(j)
            for s in range(width_dom):
                send_dom[k, j, 3 * s:3 * s + 3, :] = vec[k, dom_rows[other * width_dom + s], 0:3, :]
            copy = pltpu.make_async_remote_copy(
                src_ref=send_dom.at[k, j], dst_ref=recv_dom.at[k, j], send_sem=dom_send_sem,
                recv_sem=dom_recv_sem.at[k % 2, j], device_id=(other, b), device_id_type=MESH)
            copy.start()
            copies["dom", j] = copy
        for o in sorted(range(1, count_sub), key=lambda o: abs(2 * o - count_sub)):
            other = (b + o) % count_sub
            for s in range(width_sub):
                send_sub[k, o - 1, 3 * s:3 * s + 3, :] = vec[k, sub_rows[other * width_sub + s], 0:3, :]
            copy = pltpu.make_async_remote_copy(
                src_ref=send_sub.at[k, o - 1], dst_ref=recv_sub.at[k, o - 1], send_sem=sub_send_sem,
                recv_sem=sub_recv_sem.at[k % 2, o - 1], device_id=(a, other), device_id_type=MESH)
            copy.start()
            copies["sub", o] = copy
        for j in reversed(range(bits - 1)):
            other = partner_dom(j)
            for s in range(width_dom):
                send_dom[k, j, 3 * s:3 * s + 3, :] = vec[k, dom_rows[other * width_dom + s], 0:3, :]
            copy = pltpu.make_async_remote_copy(
                src_ref=send_dom.at[k, j], dst_ref=recv_dom.at[k, j], send_sem=dom_send_sem,
                recv_sem=dom_recv_sem.at[k % 2, j], device_id=(other, b), device_id_type=MESH)
            copy.start()
            copies["dom", j] = copy
        return copies

    def expand_own(k):
        for n in range(nb):
            expanded[n] = split_rows(vec[k, n])

    def expand_received(k, copies):
        for o in range(1, count_sub):
            copies["sub", o].wait_recv()
            base = nb + count_dom * width_dom + ((b + count_sub - o) % count_sub) * width_sub
            for s in range(width_sub):
                expanded[base + s] = split_rows(doubled(recv_sub[k, o - 1, 3 * s:3 * s + 3, :]))

    def expand_received_dom(k, copies):
        for j in rounds[k]:
            pl.semaphore_wait(far_sem.at[j], 1)
        for j in range(bits):
            copies["dom", j].wait_recv()
            base = nb + partner_dom(j) * width_dom
            for s in range(width_dom):
                expanded[base + s] = split_rows(doubled(recv_dom[k, j, 3 * s:3 * s + 3, :]))

    def multiply(left, right, matrix):
        rows = jnp.concatenate([left, right], axis=0).astype(BF16)
        out = jnp.dot(jnp.concatenate([rows, rows], axis=1), matrix, preferred_element_type=F32)
        return out[0:8, 0:tile], out[8:16, tile:2 * tile]

    def block_of(t, base):
        if base == "local":
            return local_rows[t]
        if base == "dom":
            return nb + dom_slots[t - lt]
        return nb + count_dom * width_dom + sub_slots[t - lt - ld]

    def one_pair(p, base, matrix=None):
        left, right = multiply(expanded[block_of(2 * p, base)], expanded[block_of(2 * p + 1, base)],
                               weights[p] if matrix is None else matrix)
        both = jnp.concatenate([left, right], axis=0)
        h = both.astype(BF16)
        low = (both - h.astype(F32)).astype(BF16)
        products[pl.ds(pl.multiple_of(16 * p, 16), 16), :] = jnp.concatenate([h, low], axis=1)
        return left, right

    def run_pairs(first, last, base):
        for p in range(first, last):
            one_pair(p, base)

    def scatter(first, last):
        out = jnp.dot(place[:, 8 * first:8 * last], products[8 * first:8 * last, :], preferred_element_type=F32)
        return (out[:, 0:tile] + out[:, tile:2 * tile]).reshape(nb, 8, tile)

    def apply_pre(k):
        for p in range(nb // 2):
            left, right = multiply(split_rows(image[k, 2 * p]), split_rows(image[k, 2 * p + 1]),
                                   jnp.concatenate([blocks[2 * p], blocks[2 * p + 1]], axis=1))
            left = left + pltpu.roll(left, 4, 0)
            right = right + pltpu.roll(right, 4, 0)
            if k > 0:
                left = left - SHIFT * vec[k, 2 * p]
                right = right - SHIFT * vec[k, 2 * p + 1]
            vec[k + 1, 2 * p] = left
            vec[k + 1, 2 * p + 1] = right

    with jax.named_scope('small_wait2'):
        expand_own(0)
        for copy in small[3:]:
            copy.wait()

    column = 0
    for cols in (local_cols, dom_cols, sub_cols):
        n = cols.shape[1]
        reach = (lax.broadcasted_iota(jnp.int32, (n, 8 * n), 1) // 8
                 == lax.broadcasted_iota(jnp.int32, (n, 8 * n), 0)).astype(F32).astype(BF16)
        spread = jnp.dot(jnp.broadcast_to(cols[...].astype(F32), (8, n)).astype(BF16), reach,
                         preferred_element_type=F32)
        pattern = ((lax.broadcasted_iota(jnp.int32, (8, 8 * n), 1) % 4)
                   == (lax.broadcasted_iota(jnp.int32, (8, 8 * n), 0) % 4))
        spread = jnp.where(pattern, spread, -1.0)
        for k in range(0, nb, 2):
            low = jnp.where(jnp.abs(spread - k) < 0.5, 1.0, 0.0)
            up = jnp.where(jnp.abs(spread - (k + 1)) < 0.5, 1.0, 0.0)
            place[8 * k:8 * k + 16, column:column + 8 * n] = jnp.concatenate([low, up], axis=0).astype(BF16)
        column += 8 * n

    with jax.named_scope('barrier'):
        pl.semaphore_wait(barrier, bits + count_sub - 1)
    with jax.named_scope('exch#k=0'):
        copies = [exchange(0)]
    used = live[0]

    def convert(p, masked=False):
        for side in range(2):
            value = stage[2 * p + side]
            if masked:
                value = value * (2 * p + side < used).astype(F32)
            h = value.astype(BF16)
            weights[p, 0:tile, side * tile:(side + 1) * tile] = h
            weights[p, tile:2 * tile, side * tile:(side + 1) * tile] = (value - h.astype(F32)).astype(BF16)

    def convert_group(g, masked=False):
        first, end = groups[g]

        def body(i, carry):
            for u in range(8):
                convert(first // 2 + i * 8 + u, masked)
            return carry
        lax.fori_loop(0, (end - first) // 16, body, 0)

    def convert_blocks():
        def body(i, carry):
            for u in range(16):
                value = stage[tiles + i * 16 + u]
                h = value.astype(BF16)
                blocks[i * 16 + u, 0:tile] = h
                blocks[i * 16 + u, tile:2 * tile] = (value - h.astype(F32)).astype(BF16)
            return carry
        lax.fori_loop(0, nb // 16, body, 0)

    def fuse(t):
        side = slice(t % 2 * tile, t % 2 * tile + tile)
        block = blocks[dom_cols_s[t]]
        high_part = weights[(lt + t) // 2, 0:tile, side]
        low_part = weights[(lt + t) // 2, tile:2 * tile, side]
        value = (jnp.dot(jnp.concatenate([high_part, high_part], axis=1), block, preferred_element_type=F32)
                 + jnp.dot(low_part, block[0:tile], preferred_element_type=F32))
        h = value.astype(BF16)
        fused[t // 2, 0:tile, side] = h
        fused[t // 2, tile:2 * tile, side] = (value - h.astype(F32)).astype(BF16)

    def meet(total, first, last, base, cols):
        for p in range(first, last):
            left, right = one_pair(p, base)
            total = (total + left * vec[ITERS, cols[2 * (p - first)]]
                     + right * vec[ITERS, cols[2 * (p - first) + 1]])
        return total

    def add_parts(k, first, last):
        part = scatter(first, last)
        for n in range(nb):
            image[k, n] = image[k, n] + part[n]

    def run_fused():
        for p in range(ld // 2):
            one_pair(lt // 2 + p, "dom", fused[p])

    def add_fused(k):
        part = scatter(lt, lt + ld)
        for n in range(nb):
            vec[k + 1, n] = vec[k + 1, n] + part[n]

    pairs = [(i, j) for i in range(ITERS) for j in range(i, ITERS)]

    def inner(sums):
        totals = [jnp.zeros((8, tile), F32)] * len(sums)
        for n in range(nb):
            vectors = {i: vec[i + 1, n] for i in {x for x, _ in sums}}
            images = {j: image[j, n] for j in {y for _, y in sums}}
            totals = [t + vectors[x] * images[y] for t, (x, y) in zip(totals, sums)]
        return totals

    row_of = sub8 % 4
    lane = lax.broadcasted_iota(jnp.int32, (8, tile), 1)
    span = tile // 4
    last = ITERS - 1
    order = [(i, 0) for i in range(ITERS)] + [(j, i + 1) for i, j in pairs if i < last]

    def share(which, packed):
        own[which] = jnp.sum(packed, axis=0, keepdims=True)
        for o in reversed(range(1, count_dom * count_sub)):
            target = ((a + o // count_sub) % count_dom, (b + o % count_sub) % count_sub)
            copy = pltpu.make_async_remote_copy(
                src_ref=own.at[which], dst_ref=sums.at[which, o - 1], send_sem=red_send,
                recv_sem=red_recv.at[which], device_id=target, device_id_type=MESH)
            copy.start()

    def shared(which):
        drain(sums.at[which], red_recv.at[which])
        parts = [own[which]] + [sums[which, o] for o in range(count_dom * count_sub - 1)]
        while len(parts) > 1:
            parts = [x + y for x, y in zip(parts[::2], parts[1::2])] + (parts[-1:] if len(parts) % 2 else [])
        return jnp.broadcast_to(parts[0], (8, tile))

    def pick(row, i):
        mine = jnp.where(lane == span * row_of + i, row, 0.0)
        return jnp.sum(mine, axis=1, keepdims=True) + jnp.zeros((8, tile), F32)

    rounds = [range(0, 0)] + [range((k - 1) * bits // ITERS, k * bits // ITERS) for k in range(1, ITERS + 1)]
    for k in range(ITERS + 1):
        if k > 0:
            with jax.named_scope(f'exch#k={k}'):
                copies.append(exchange(k))
                for j in rounds[k]:
                    pl.semaphore_signal(far_sem.at[j], inc=1, device_id=(partner_dom(j), b), device_id_type=MESH)
            with jax.named_scope(f'own#k={k}'):
                expand_own(k)
                if k > 1:
                    run_pairs(lt // 2, (lt + ld) // 2, "dom")
                run_pairs(0, lt // 2, "local")
                if k > 1:
                    add_parts(k - 1, lt, lt + ld)
        else:
            with jax.named_scope('arrive_local'):
                loaded(0)
                convert_group(0, True)
                loaded(1)
                convert_group(1, True)
                loaded(2)
                run_pairs(0, lt // 2, "local")
                for p in range((lt + ld) // 2, tiles // 2):
                    convert(p)
        part = scatter(0, lt)
        for n in range(nb):
            if k > 0:
                image[k, n] = part[n] + mass_ref[n:n + 1, :] * vec[k, n]
            else:
                image[k, n] = part[n]
        if k == ITERS:
            packed = jnp.zeros((8, tile), F32)
            for i, total in enumerate(inner(order)):
                value = jnp.sum(total, axis=1, keepdims=True)
                packed = jnp.where((lane == span * row_of + i) & (sub8 < 3), value, packed)
            share(0, packed)
        if k == 1 and ITERS > 1:
            with jax.named_scope('fuse'):
                for t in range(ld):
                    fuse(t)
        if k == 0:
            with jax.named_scope('arrive_rest'):
                loaded(3)
                convert_group(3)
                loaded(4)
                convert_blocks()
        if k == ITERS:
            late = jnp.where(upper, inner([(last, ITERS)])[0], 0.0)
        with jax.named_scope(f'recvsub#k={k}'):
            expand_received(k, copies[k])
        with jax.named_scope(f'runsub#k={k}'):
            if k == ITERS:
                late = meet(late, (lt + ld) // 2, tiles // 2, "sub", sub_cols_s)
            else:
                run_pairs((lt + ld) // 2, tiles // 2, "sub")
        if 0 < k < ITERS:
            @pl.when(b % 2 == 0)
            def _(k=k):
                with jax.named_scope(f'pre#k={k}'):
                    add_parts(k, lt + ld, tiles)
                    apply_pre(k)
                with jax.named_scope(f'recvdom#k={k}'):
                    expand_received_dom(k, copies[k])
                with jax.named_scope(f'rundom#k={k}'):
                    run_fused()
                    add_fused(k)

            @pl.when(b % 2 == 1)
            def _(k=k):
                with jax.named_scope(f'recvdom#k={k}'):
                    expand_received_dom(k, copies[k])
                with jax.named_scope(f'rundom#k={k}'):
                    run_fused()
                    add_parts(k, lt + ld, tiles)
                    apply_pre(k)
                    add_fused(k)
            continue
        with jax.named_scope(f'recvdom#k={k}'):
            expand_received_dom(k, copies[k])
        with jax.named_scope(f'rundom#k={k}'):
            if k == 0:
                run_pairs(lt // 2, (lt + ld) // 2, "dom")
                part = scatter(lt, tiles)
                for n in range(nb):
                    image[k, n] = -(image[k, n] + part[n])
                apply_pre(k)
            else:
                late = meet(late, lt // 2, (lt + ld) // 2, "dom", dom_cols_s)
                value = jnp.sum(late, axis=1, keepdims=True)
                share(1, jnp.where((lane == span * row_of) & (row_of < 3), value, 0.0))
                add_parts(k, lt, tiles)

    with jax.named_scope('red0_wait'):
        row = shared(0)
    gram = {}
    for i, pair in enumerate(order[ITERS:]):
        gram[pair[0], pair[1] - 1] = gram[pair[1] - 1, pair[0]] = pick(row, ITERS + i)
    first = [pick(row, i) for i in range(ITERS)]

    def add(x, y):
        return y if x is None else x if y is None else x + y

    direction = [jnp.ones((8, tile), F32)] + [None] * (ITERS - 1)
    coefs = [None] * ITERS
    current = first[0]
    for it in range(ITERS):
        used_terms = [i for i in range(ITERS) if direction[i] is not None]
        curvature = None
        for i in used_terms:
            inner_sum = None
            for j in used_terms:
                if (i, j) in gram:
                    inner_sum = add(inner_sum, gram[i, j] * direction[j])
            curvature = add(curvature, direction[i] * inner_sum)
        if it == last:
            break
        step = current / curvature
        for i in used_terms:
            coefs[i] = add(coefs[i], step * direction[i])
        if it + 1 < ITERS:
            smooth = [jnp.ones((8, tile), F32)] + [None] * (ITERS - 1)
            for j in range(it + 1):
                smooth[j + 1] = add(smooth[j + 1], -coefs[j])
                smooth[j] = add(smooth[j], -SHIFT * coefs[j])
            following = None
            for i in range(ITERS):
                if smooth[i] is None:
                    continue
                inner = first[i]
                for j in range(it + 1):
                    inner = inner - coefs[j] * gram[i, j]
                following = add(following, smooth[i] * inner)
            ratio = following / current
            direction = [add(s, None if d is None else ratio * d) for s, d in zip(smooth, direction)]
            current = following

    for n in range(nb):
        x, r, along, image_along = vec[0, n], image[0, n], None, None
        for i in range(ITERS):
            if coefs[i] is not None:
                x = x + coefs[i] * vec[i + 1, n]
                r = r - coefs[i] * image[i + 1, n]
            along = add(along, direction[i] * vec[i + 1, n])
            image_along = add(image_along, direction[i] * image[i + 1, n])
        vec[0, n], image[0, n], vec[1, n], image[1, n] = x, r, along, image_along

    with jax.named_scope('red1_wait'):
        row = shared(1)
    step = current / (curvature + direction[last] * direction[last] * pick(row, 0))
    for n in range(nb):
        x = vec[0, n] + step * vec[1, n]
        r = image[0, n] - step * image[1, n]
        sol_ref[:, n * tile:(n + 1) * tile] = x[0:3, :]
        res_ref[:, n * tile:(n + 1) * tile] = r[0:3, :]

    with jax.named_scope('send_wait'):
        drain(send_sub, sub_send_sem)
        drain(send_dom, dom_send_sem)
        drain(sums, red_send)


def finish(sol_in, res_in, sol_ref, res_ref):
    sol_ref[...] = sol_in[...]
    res_ref[...] = res_in[...]


def on_device(positions, mass, local_tiles, local_rows, local_cols, live_tiles, dom_tiles, dom_cols, dom_slots,
              dom_rows, sub_tiles, sub_cols, sub_slots, sub_rows, precond):
    count_dom = lax.axis_size("dom")
    count_sub = lax.axis_size("sub")
    bits = count_dom.bit_length() - 1
    nb, tile = precond.shape[0], precond.shape[1]
    lt, ld, ls = local_tiles.shape[0], dom_tiles.shape[0], sub_tiles.shape[0]
    tiles = lt + ld + ls
    width_dom = dom_rows.shape[0] // count_dom
    width_sub = sub_rows.shape[0] // count_sub
    vmem = pl.BlockSpec(memory_space=pltpu.VMEM)
    anym = pl.BlockSpec(memory_space=pltpu.HBM)
    k = ITERS + 1
    n_red = count_dom * count_sub - 1
    outs = pl.pallas_call(
        functools.partial(kernel, count_dom, count_sub, bits),
        out_shape=[pltpu.VMEM(positions.shape, F32)] * 2,
        in_specs=[anym] * 17,
        out_specs=[vmem, vmem],
        scratch_shapes=[
            pltpu.VMEM((tiles + nb, tile, tile), F32),
            pltpu.VMEM((tiles // 2, 2 * tile, 2 * tile), BF16),
            pltpu.VMEM((8 * nb, 8 * tiles), BF16),
            pltpu.VMEM((k, nb, 8, tile), F32),
            pltpu.VMEM((k, nb, 8, tile), F32),
            pltpu.VMEM((nb + count_dom * width_dom + count_sub * width_sub, 8, tile), F32),
            pltpu.VMEM((8 * tiles, 2 * tile), BF16),
            pltpu.SMEM(local_rows.shape, jnp.int32),
            pltpu.SMEM(live_tiles.shape, jnp.int32),
            pltpu.SMEM(dom_rows.shape, jnp.int32),
            pltpu.SMEM(dom_slots.shape, jnp.int32),
            pltpu.SMEM(sub_rows.shape, jnp.int32),
            pltpu.SMEM(sub_slots.shape, jnp.int32),
            pltpu.SMEM(dom_cols.shape, jnp.int32),
            pltpu.SMEM(sub_cols.shape, jnp.int32),
            pltpu.VMEM((k, bits, 3 * width_dom, tile), F32),
            pltpu.VMEM((k, bits, 3 * width_dom, tile), F32),
            pltpu.VMEM((k, count_sub - 1, 3 * width_sub, tile), F32),
            pltpu.VMEM((k, count_sub - 1, 3 * width_sub, tile), F32),
            pltpu.VMEM((2, count_dom * count_sub - 1, 1, tile), F32),
            pltpu.VMEM((2, 1, tile), F32),
            pltpu.SemaphoreType.DMA((5,)),
            pltpu.SemaphoreType.DMA,
            pltpu.SemaphoreType.DMA((2, bits)),
            pltpu.SemaphoreType.DMA,
            pltpu.SemaphoreType.DMA((2, count_sub - 1)),
            pltpu.SemaphoreType.DMA,
            pltpu.SemaphoreType.DMA((2,)),
            pltpu.VMEM(positions.shape, F32),
            pltpu.VMEM((nb, tile), F32),
            pltpu.VMEM((1, lt), jnp.int32),
            pltpu.VMEM((1, ld), jnp.int32),
            pltpu.VMEM((1, ls), jnp.int32),
            pltpu.SemaphoreType.DMA((4,)),
            pltpu.SemaphoreType.REGULAR((bits,)),
            pltpu.VMEM((ld // 2, 2 * tile, 2 * tile), BF16),
            pltpu.VMEM((nb, 2 * tile, tile), BF16),
        ],
        compiler_params=pltpu.CompilerParams(
            collective_id=0, has_side_effects=True, vmem_limit_bytes=62914560),
        name="fairing",
    )(positions, mass.reshape(nb, tile), local_rows, live_tiles, dom_rows, dom_slots, sub_rows, sub_slots, dom_cols, sub_cols,
      local_cols.reshape(1, lt), dom_cols.reshape(1, ld), sub_cols.reshape(1, ls),
      local_tiles, dom_tiles, sub_tiles, precond)
    return pl.pallas_call(
        finish,
        out_shape=[jax.ShapeDtypeStruct(positions.shape, F32)] * 2,
        in_specs=[vmem, vmem],
        out_specs=[vmem, vmem],
        compiler_params=pltpu.CompilerParams(vmem_limit_bytes=8388608),
        name="finish",
    )(*outs)


def solution(mesh):
    split = P(("dom", "sub"))
    tiled = P(("dom", "sub"), None, None)
    placed = (P(None, ("dom", "sub")), split, tiled, split, split, split, tiled, split, split, split, tiled, split,
              split, split, tiled)
    return jax.shard_map(
        on_device,
        mesh=mesh,
        in_specs=placed,
        out_specs=(P(None, ("dom", "sub")), P(None, ("dom", "sub"))),
        check_vma=False,
    )
```

```python
import functools

import jax
import jax.numpy as jnp
from jax import lax
from jax.experimental import pallas as pl
from jax.experimental.pallas import tpu as pltpu
from jax.sharding import PartitionSpec as P

ITERS = 3
SHIFT = 1.0
CHUNK = 16
F32 = jnp.float32
BF16 = jnp.bfloat16
MESH = pl.DeviceIdType.MESH


def high(value):
    return value.astype(BF16).astype(F32)


def drain(ref, sem):
    pltpu.make_async_copy(ref, ref, sem).wait()


def kernel(count_dom, count_sub, bits, pos_hbm, mass_hbm, local_rows_hbm, live_hbm, dom_rows_hbm, dom_slots_hbm,
           sub_rows_hbm, sub_slots_hbm, dom_cols_flat, sub_cols_flat, local_cols_hbm, dom_cols_hbm, sub_cols_hbm, local_hbm, dom_hbm, sub_hbm, pre_hbm, sol_ref, res_ref,
           stage, weights, place, vec, image, expanded, products, local_rows, live, dom_rows, dom_slots, sub_rows,
           sub_slots, dom_cols_s, sub_cols_s, send_dom, recv_dom, send_sub, recv_sub,
           sums, own, load_sem, dom_send_sem, dom_recv_sem, sub_send_sem, sub_recv_sem,
           red_send, red_recv, pos_ref, mass_ref, local_cols, dom_cols, sub_cols,
           small_sem, far_sem, fused, blocks):
    lt, ld, ls, nb = local_hbm.shape[0], dom_hbm.shape[0], sub_hbm.shape[0], pre_hbm.shape[0]
    tile = pre_hbm.shape[1]
    width_dom = dom_rows_hbm.shape[0] // count_dom
    width_sub = sub_rows_hbm.shape[0] // count_sub
    a = lax.axis_index("dom")
    b = lax.axis_index("sub")
    tiles = lt + ld + ls

    def partner_dom(j):
        bit = 1 << j
        return a + bit - 2 * bit * ((a // bit) % 2)

    small = []
    for source, target in ((pos_hbm, pos_ref), (dom_rows_hbm, dom_rows), (sub_rows_hbm, sub_rows),
                           (local_cols_hbm, local_cols), (dom_cols_hbm, dom_cols), (sub_cols_hbm, sub_cols),
                           (local_rows_hbm, local_rows), (live_hbm, live), (sub_slots_hbm, sub_slots),
                           (dom_slots_hbm, dom_slots), (mass_hbm, mass_ref), (dom_cols_flat, dom_cols_s), (sub_cols_flat, sub_cols_s)):
        copy = pltpu.make_async_copy(source, target, small_sem.at[min(len(small), 3)])
        copy.start()
        small.append(copy)

    barrier = pltpu.get_barrier_semaphore()
    for j in reversed(range(bits)):
        pl.semaphore_signal(barrier, inc=1, device_id=(partner_dom(j), b), device_id_type=MESH)
    for o in range(1, count_sub):
        pl.semaphore_signal(barrier, inc=1, device_id=(a, (b + o) % count_sub), device_id_type=MESH)

    groups = ((0, 2 * CHUNK), (2 * CHUNK, lt), (lt + ld, tiles), (lt, lt + ld), (tiles, tiles + nb))
    sources = (local_hbm, local_hbm, sub_hbm, dom_hbm, pre_hbm)
    for g, ((first, end), source) in enumerate(zip(groups, sources)):
        offset = first if g < 2 else 0
        for c in range(0, end - first, CHUNK):
            pltpu.make_async_copy(source.at[pl.ds(offset + c, CHUNK)], stage.at[pl.ds(first + c, CHUNK)],
                                  load_sem.at[g]).start()

    def loaded(g):
        first, end = groups[g]
        drain(stage.at[pl.ds(first, end - first)], load_sem.at[g])

    sub8 = lax.broadcasted_iota(jnp.int32, (8, tile), 0)
    upper = sub8 < 4
    zero1 = jnp.zeros((1, tile), F32)

    def doubled(three):
        return jnp.concatenate([three, zero1, three, zero1], axis=0)

    def split_rows(value):
        h = high(value)
        return jnp.where(upper, h, value - h)

    with jax.named_scope('small_wait'):
        for copy in small[:3]:
            copy.wait()

    for k in range(nb):
        vec[0, k] = doubled(pos_ref[:, k * tile:(k + 1) * tile])

    def exchange(k):
        copies = {}
        for j in [bits - 1]:
            other = partner_dom(j)
            for s in range(width_dom):
                send_dom[k, j, 3 * s:3 * s + 3, :] = vec[k, dom_rows[other * width_dom + s], 0:3, :]
            copy = pltpu.make_async_remote_copy(
                src_ref=send_dom.at[k, j], dst_ref=recv_dom.at[k, j], send_sem=dom_send_sem,
                recv_sem=dom_recv_sem.at[k % 2, j], device_id=(other, b), device_id_type=MESH)
            copy.start()
            copies["dom", j] = copy
        for o in sorted(range(1, count_sub), key=lambda o: abs(2 * o - count_sub)):
            other = (b + o) % count_sub
            for s in range(width_sub):
                send_sub[k, o - 1, 3 * s:3 * s + 3, :] = vec[k, sub_rows[other * width_sub + s], 0:3, :]
            copy = pltpu.make_async_remote_copy(
                src_ref=send_sub.at[k, o - 1], dst_ref=recv_sub.at[k, o - 1], send_sem=sub_send_sem,
                recv_sem=sub_recv_sem.at[k % 2, o - 1], device_id=(a, other), device_id_type=MESH)
            copy.start()
            copies["sub", o] = copy
        for j in reversed(range(bits - 1)):
            other = partner_dom(j)
            for s in range(width_dom):
                send_dom[k, j, 3 * s:3 * s + 3, :] = vec[k, dom_rows[other * width_dom + s], 0:3, :]
            copy = pltpu.make_async_remote_copy(
                src_ref=send_dom.at[k, j], dst_ref=recv_dom.at[k, j], send_sem=dom_send_sem,
                recv_sem=dom_recv_sem.at[k % 2, j], device_id=(other, b), device_id_type=MESH)
            copy.start()
            copies["dom", j] = copy
        return copies

    def expand_own(k):
        for n in range(nb):
            expanded[n] = split_rows(vec[k, n])

    def expand_received(k, copies):
        for o in range(1, count_sub):
            copies["sub", o].wait_recv()
            base = nb + count_dom * width_dom + ((b + count_sub - o) % count_sub) * width_sub
            for s in range(width_sub):
                expanded[base + s] = split_rows(doubled(recv_sub[k, o - 1, 3 * s:3 * s + 3, :]))

    def expand_received_dom(k, copies):
        for j in rounds[k]:
            pl.semaphore_wait(far_sem.at[j], 1)
        for j in range(bits):
            copies["dom", j].wait_recv()
            base = nb + partner_dom(j) * width_dom
            for s in range(width_dom):
                expanded[base + s] = split_rows(doubled(recv_dom[k, j, 3 * s:3 * s + 3, :]))

    def multiply(left, right, matrix):
        rows = jnp.concatenate([left, right], axis=0).astype(BF16)
        out = jnp.dot(jnp.concatenate([rows, rows], axis=1), matrix, preferred_element_type=F32)
        return out[0:8, 0:tile], out[8:16, tile:2 * tile]

    def block_of(t, base):
        if base == "local":
            return local_rows[t]
        if base == "dom":
            return nb + dom_slots[t - lt]
        return nb + count_dom * width_dom + sub_slots[t - lt - ld]

    def one_pair(p, base, matrix=None):
        left, right = multiply(expanded[block_of(2 * p, base)], expanded[block_of(2 * p + 1, base)],
                               weights[p] if matrix is None else matrix)
        both = jnp.concatenate([left, right], axis=0)
        h = both.astype(BF16)
        low = (both - h.astype(F32)).astype(BF16)
        products[pl.ds(pl.multiple_of(16 * p, 16), 16), :] = jnp.concatenate([h, low], axis=1)
        return left, right

    def run_pairs(first, last, base):
        for p in range(first, last):
            one_pair(p, base)

    def scatter(first, last):
        out = jnp.dot(place[:, 8 * first:8 * last], products[8 * first:8 * last, :], preferred_element_type=F32)
        return (out[:, 0:tile] + out[:, tile:2 * tile]).reshape(nb, 8, tile)

    def apply_pre(k):
        for p in range(nb // 2):
            left, right = multiply(split_rows(image[k, 2 * p]), split_rows(image[k, 2 * p + 1]),
                                   jnp.concatenate([blocks[2 * p], blocks[2 * p + 1]], axis=1))
            left = left + pltpu.roll(left, 4, 0)
            right = right + pltpu.roll(right, 4, 0)
            if k > 0:
                left = left - SHIFT * vec[k, 2 * p]
                right = right - SHIFT * vec[k, 2 * p + 1]
            vec[k + 1, 2 * p] = left
            vec[k + 1, 2 * p + 1] = right

    with jax.named_scope('small_wait2'):
        expand_own(0)
        for copy in small[3:]:
            copy.wait()

    column = 0
    for cols in (local_cols, dom_cols, sub_cols):
        n = cols.shape[1]
        reach = (lax.broadcasted_iota(jnp.int32, (n, 8 * n), 1) // 8
                 == lax.broadcasted_iota(jnp.int32, (n, 8 * n), 0)).astype(F32).astype(BF16)
        spread = jnp.dot(jnp.broadcast_to(cols[...].astype(F32), (8, n)).astype(BF16), reach,
                         preferred_element_type=F32)
        pattern = ((lax.broadcasted_iota(jnp.int32, (8, 8 * n), 1) % 4)
                   == (lax.broadcasted_iota(jnp.int32, (8, 8 * n), 0) % 4))
        if column == 0:
            pattern = pattern & (lax.broadcasted_iota(jnp.int32, (8, 8 * n), 1) < 8 * live[0])
        spread = jnp.where(pattern, spread, -1.0)
        for k in range(0, nb, 2):
            low = jnp.where(spread == k, 1.0, 0.0)
            up = jnp.where(spread == k + 1, 1.0, 0.0)
            place[8 * k:8 * k + 16, column:column + 8 * n] = jnp.concatenate([low, up], axis=0).astype(BF16)
        column += 8 * n

    with jax.named_scope('barrier'):
        pl.semaphore_wait(barrier, bits + count_sub - 1)
    with jax.named_scope('exch#k=0'):
        copies = [exchange(0)]
    def convert(p):
        for side in range(2):
            value = stage[2 * p + side]
            h = value.astype(BF16)
            weights[p, 0:tile, side * tile:(side + 1) * tile] = h
            weights[p, tile:2 * tile, side * tile:(side + 1) * tile] = (value - h.astype(F32)).astype(BF16)

    def convert_group(g):
        first, end = groups[g]

        def body(i, carry):
            for u in range(8):
                convert(first // 2 + i * 8 + u)
            return carry
        lax.fori_loop(0, (end - first) // 16, body, 0)

    def convert_blocks():
        def body(i, carry):
            for u in range(16):
                value = stage[tiles + i * 16 + u]
                h = value.astype(BF16)
                blocks[i * 16 + u, 0:tile] = h
                blocks[i * 16 + u, tile:2 * tile] = (value - h.astype(F32)).astype(BF16)
            return carry
        lax.fori_loop(0, nb // 16, body, 0)

    def fuse(t):
        side = slice(t % 2 * tile, t % 2 * tile + tile)
        block = blocks[dom_cols_s[t]]
        high_part = weights[(lt + t) // 2, 0:tile, side]
        low_part = weights[(lt + t) // 2, tile:2 * tile, side]
        value = (jnp.dot(jnp.concatenate([high_part, high_part], axis=1), block, preferred_element_type=F32)
                 + jnp.dot(low_part, block[0:tile], preferred_element_type=F32))
        h = value.astype(BF16)
        fused[t // 2, 0:tile, side] = h
        fused[t // 2, tile:2 * tile, side] = (value - h.astype(F32)).astype(BF16)

    def meet(total, first, last, base, cols):
        for p in range(first, last):
            left, right = one_pair(p, base)
            total = (total + left * vec[ITERS, cols[2 * (p - first)]]
                     + right * vec[ITERS, cols[2 * (p - first) + 1]])
        return total

    def add_parts(k, first, last):
        part = scatter(first, last)
        for n in range(nb):
            image[k, n] = image[k, n] + part[n]

    def run_fused():
        for p in range(ld // 2):
            one_pair(lt // 2 + p, "dom", fused[p])

    def add_fused(k):
        part = scatter(lt, lt + ld)
        for n in range(nb):
            vec[k + 1, n] = vec[k + 1, n] + part[n]

    pairs = [(i, j) for i in range(ITERS) for j in range(i, ITERS)]

    def inner(sums):
        totals = [jnp.zeros((8, tile), F32)] * len(sums)
        for n in range(nb):
            vectors = {i: vec[i + 1, n] for i in {x for x, _ in sums}}
            images = {j: image[j, n] for j in {y for _, y in sums}}
            totals = [t + vectors[x] * images[y] for t, (x, y) in zip(totals, sums)]
        return totals

    row_of = sub8 % 4
    lane = lax.broadcasted_iota(jnp.int32, (8, tile), 1)
    span = tile // 4
    last = ITERS - 1
    order = [(i, 0) for i in range(ITERS)] + [(j, i + 1) for i, j in pairs if i < last]

    def share(which, packed):
        own[which] = jnp.sum(packed, axis=0, keepdims=True)
        for o in reversed(range(1, count_dom * count_sub)):
            target = ((a + o // count_sub) % count_dom, (b + o % count_sub) % count_sub)
            copy = pltpu.make_async_remote_copy(
                src_ref=own.at[which], dst_ref=sums.at[which, o - 1], send_sem=red_send,
                recv_sem=red_recv.at[which], device_id=target, device_id_type=MESH)
            copy.start()

    def shared(which):
        drain(sums.at[which], red_recv.at[which])
        parts = [own[which]] + [sums[which, o] for o in range(count_dom * count_sub - 1)]
        while len(parts) > 1:
            parts = [x + y for x, y in zip(parts[::2], parts[1::2])] + (parts[-1:] if len(parts) % 2 else [])
        return jnp.broadcast_to(parts[0], (8, tile))

    def pick(row, i):
        mine = jnp.where(lane == span * row_of + i, row, 0.0)
        return jnp.sum(mine, axis=1, keepdims=True) + jnp.zeros((8, tile), F32)

    rounds = [range(0, 0)] + [range((k - 1) * bits // ITERS, k * bits // ITERS) for k in range(1, ITERS + 1)]
    for k in range(ITERS + 1):
        if k > 0:
            with jax.named_scope(f'exch#k={k}'):
                copies.append(exchange(k))
                for j in rounds[k]:
                    pl.semaphore_signal(far_sem.at[j], inc=1, device_id=(partner_dom(j), b), device_id_type=MESH)
            with jax.named_scope(f'own#k={k}'):
                expand_own(k)
                if k > 1:
                    run_pairs(lt // 2, (lt + ld) // 2, "dom")
                run_pairs(0, lt // 2, "local")
                if k > 1:
                    add_parts(k - 1, lt, lt + ld)
        else:
            with jax.named_scope('arrive_local'):
                loaded(0)
                convert_group(0)
                loaded(1)
                convert_group(1)
                loaded(2)
                run_pairs(0, lt // 2, "local")
                for p in range((lt + ld) // 2, tiles // 2):
                    convert(p)
        part = scatter(0, lt)
        for n in range(nb):
            if k > 0:
                image[k, n] = part[n] + mass_ref[n:n + 1, :] * vec[k, n]
            else:
                image[k, n] = part[n]
        if k == ITERS:
            packed = jnp.zeros((8, tile), F32)
            for i, total in enumerate(inner(order)):
                value = jnp.sum(total, axis=1, keepdims=True)
                packed = jnp.where((lane == span * row_of + i) & (sub8 < 3), value, packed)
            share(0, packed)
        if k == 1 and ITERS > 1:
            with jax.named_scope('fuse'):
                for t in range(ld):
                    fuse(t)
        if k == 0:
            with jax.named_scope('arrive_rest'):
                loaded(3)
                convert_group(3)
                loaded(4)
                convert_blocks()
        if k == ITERS:
            late = jnp.where(upper, inner([(last, ITERS)])[0], 0.0)
        with jax.named_scope(f'recvsub#k={k}'):
            expand_received(k, copies[k])
        with jax.named_scope(f'runsub#k={k}'):
            if k == ITERS:
                late = meet(late, (lt + ld) // 2, tiles // 2, "sub", sub_cols_s)
            else:
                run_pairs((lt + ld) // 2, tiles // 2, "sub")
        if 0 < k < ITERS:
            @pl.when(b % 2 == 0)
            def _(k=k):
                with jax.named_scope(f'pre#k={k}'):
                    add_parts(k, lt + ld, tiles)
                    apply_pre(k)
                with jax.named_scope(f'recvdom#k={k}'):
                    expand_received_dom(k, copies[k])
                with jax.named_scope(f'rundom#k={k}'):
                    run_fused()
                    add_fused(k)

            @pl.when(b % 2 == 1)
            def _(k=k):
                with jax.named_scope(f'recvdom#k={k}'):
                    expand_received_dom(k, copies[k])
                with jax.named_scope(f'rundom#k={k}'):
                    run_fused()
                    add_parts(k, lt + ld, tiles)
                    apply_pre(k)
                    add_fused(k)
            continue
        with jax.named_scope(f'recvdom#k={k}'):
            expand_received_dom(k, copies[k])
        with jax.named_scope(f'rundom#k={k}'):
            if k == 0:
                run_pairs(lt // 2, (lt + ld) // 2, "dom")
                part = scatter(lt, tiles)
                for n in range(nb):
                    image[k, n] = -(image[k, n] + part[n])
                apply_pre(k)
            else:
                late = meet(late, lt // 2, (lt + ld) // 2, "dom", dom_cols_s)
                value = jnp.sum(late, axis=1, keepdims=True)
                share(1, jnp.where((lane == span * row_of) & (row_of < 3), value, 0.0))
                add_parts(k, lt, tiles)

    with jax.named_scope('red0_wait'):
        row = shared(0)
    gram = {}
    for i, pair in enumerate(order[ITERS:]):
        gram[pair[0], pair[1] - 1] = gram[pair[1] - 1, pair[0]] = pick(row, ITERS + i)
    first = [pick(row, i) for i in range(ITERS)]

    def add(x, y):
        return y if x is None else x if y is None else x + y

    direction = [jnp.ones((8, tile), F32)] + [None] * (ITERS - 1)
    coefs = [None] * ITERS
    current = first[0]
    for it in range(ITERS):
        used_terms = [i for i in range(ITERS) if direction[i] is not None]
        curvature = None
        for i in used_terms:
            inner_sum = None
            for j in used_terms:
                if (i, j) in gram:
                    inner_sum = add(inner_sum, gram[i, j] * direction[j])
            curvature = add(curvature, direction[i] * inner_sum)
        if it == last:
            break
        step = current / curvature
        for i in used_terms:
            coefs[i] = add(coefs[i], step * direction[i])
        if it + 1 < ITERS:
            smooth = [jnp.ones((8, tile), F32)] + [None] * (ITERS - 1)
            for j in range(it + 1):
                smooth[j + 1] = add(smooth[j + 1], -coefs[j])
                smooth[j] = add(smooth[j], -SHIFT * coefs[j])
            following = None
            for i in range(ITERS):
                if smooth[i] is None:
                    continue
                inner = first[i]
                for j in range(it + 1):
                    inner = inner - coefs[j] * gram[i, j]
                following = add(following, smooth[i] * inner)
            ratio = following / current
            direction = [add(s, None if d is None else ratio * d) for s, d in zip(smooth, direction)]
            current = following

    for n in range(nb):
        x, r, along, image_along = vec[0, n], image[0, n], None, None
        for i in range(ITERS):
            if coefs[i] is not None:
                x = x + coefs[i] * vec[i + 1, n]
                r = r - coefs[i] * image[i + 1, n]
            along = add(along, direction[i] * vec[i + 1, n])
            image_along = add(image_along, direction[i] * image[i + 1, n])
        vec[0, n], image[0, n], vec[1, n], image[1, n] = x, r, along, image_along

    with jax.named_scope('red1_wait'):
        row = shared(1)
    step = current / (curvature + direction[last] * direction[last] * pick(row, 0))
    for n in range(nb):
        x = vec[0, n] + step * vec[1, n]
        r = image[0, n] - step * image[1, n]
        sol_ref[:, n * tile:(n + 1) * tile] = x[0:3, :]
        res_ref[:, n * tile:(n + 1) * tile] = r[0:3, :]

    with jax.named_scope('send_wait'):
        drain(send_sub, sub_send_sem)
        drain(send_dom, dom_send_sem)
        drain(sums, red_send)


def finish(sol_in, res_in, sol_ref, res_ref):
    sol_ref[...] = sol_in[...]
    res_ref[...] = res_in[...]


def on_device(positions, mass, local_tiles, local_rows, local_cols, live_tiles, dom_tiles, dom_cols, dom_slots,
              dom_rows, sub_tiles, sub_cols, sub_slots, sub_rows, precond):
    count_dom = lax.axis_size("dom")
    count_sub = lax.axis_size("sub")
    bits = count_dom.bit_length() - 1
    nb, tile = precond.shape[0], precond.shape[1]
    lt, ld, ls = local_tiles.shape[0], dom_tiles.shape[0], sub_tiles.shape[0]
    tiles = lt + ld + ls
    width_dom = dom_rows.shape[0] // count_dom
    width_sub = sub_rows.shape[0] // count_sub
    vmem = pl.BlockSpec(memory_space=pltpu.VMEM)
    anym = pl.BlockSpec(memory_space=pltpu.HBM)
    k = ITERS + 1
    n_red = count_dom * count_sub - 1
    outs = pl.pallas_call(
        functools.partial(kernel, count_dom, count_sub, bits),
        out_shape=[pltpu.VMEM(positions.shape, F32)] * 2,
        in_specs=[anym] * 17,
        out_specs=[vmem, vmem],
        scratch_shapes=[
            pltpu.VMEM((tiles + nb, tile, tile), F32),
            pltpu.VMEM((tiles // 2, 2 * tile, 2 * tile), BF16),
            pltpu.VMEM((8 * nb, 8 * tiles), BF16),
            pltpu.VMEM((k, nb, 8, tile), F32),
            pltpu.VMEM((k, nb, 8, tile), F32),
            pltpu.VMEM((nb + count_dom * width_dom + count_sub * width_sub, 8, tile), F32),
            pltpu.VMEM((8 * tiles, 2 * tile), BF16),
            pltpu.SMEM(local_rows.shape, jnp.int32),
            pltpu.SMEM(live_tiles.shape, jnp.int32),
            pltpu.SMEM(dom_rows.shape, jnp.int32),
            pltpu.SMEM(dom_slots.shape, jnp.int32),
            pltpu.SMEM(sub_rows.shape, jnp.int32),
            pltpu.SMEM(sub_slots.shape, jnp.int32),
            pltpu.SMEM(dom_cols.shape, jnp.int32),
            pltpu.SMEM(sub_cols.shape, jnp.int32),
            pltpu.VMEM((k, bits, 3 * width_dom, tile), F32),
            pltpu.VMEM((k, bits, 3 * width_dom, tile), F32),
            pltpu.VMEM((k, count_sub - 1, 3 * width_sub, tile), F32),
            pltpu.VMEM((k, count_sub - 1, 3 * width_sub, tile), F32),
            pltpu.VMEM((2, count_dom * count_sub - 1, 1, tile), F32),
            pltpu.VMEM((2, 1, tile), F32),
            pltpu.SemaphoreType.DMA((5,)),
            pltpu.SemaphoreType.DMA,
            pltpu.SemaphoreType.DMA((2, bits)),
            pltpu.SemaphoreType.DMA,
            pltpu.SemaphoreType.DMA((2, count_sub - 1)),
            pltpu.SemaphoreType.DMA,
            pltpu.SemaphoreType.DMA((2,)),
            pltpu.VMEM(positions.shape, F32),
            pltpu.VMEM((nb, tile), F32),
            pltpu.VMEM((1, lt), jnp.int32),
            pltpu.VMEM((1, ld), jnp.int32),
            pltpu.VMEM((1, ls), jnp.int32),
            pltpu.SemaphoreType.DMA((4,)),
            pltpu.SemaphoreType.REGULAR((bits,)),
            pltpu.VMEM((ld // 2, 2 * tile, 2 * tile), BF16),
            pltpu.VMEM((nb, 2 * tile, tile), BF16),
        ],
        compiler_params=pltpu.CompilerParams(
            collective_id=0, has_side_effects=True, vmem_limit_bytes=62914560),
        name="fairing",
    )(positions, mass.reshape(nb, tile), local_rows, live_tiles, dom_rows, dom_slots, sub_rows, sub_slots, dom_cols, sub_cols,
      local_cols.reshape(1, lt), dom_cols.reshape(1, ld), sub_cols.reshape(1, ls),
      local_tiles, dom_tiles, sub_tiles, precond)
    return pl.pallas_call(
        finish,
        out_shape=[jax.ShapeDtypeStruct(positions.shape, F32)] * 2,
        in_specs=[vmem, vmem],
        out_specs=[vmem, vmem],
        compiler_params=pltpu.CompilerParams(vmem_limit_bytes=8388608),
        name="finish",
    )(*outs)


def solution(mesh):
    split = P(("dom", "sub"))
    tiled = P(("dom", "sub"), None, None)
    placed = (P(None, ("dom", "sub")), split, tiled, split, split, split, tiled, split, split, split, tiled, split,
              split, split, tiled)
    return jax.shard_map(
        on_device,
        mesh=mesh,
        in_specs=placed,
        out_specs=(P(None, ("dom", "sub")), P(None, ("dom", "sub"))),
        check_vma=False,
    )
```
